32 devices in a mesh: wide: 16 (over z, y, core), narrow: 2 (over x).
Axes of the slice: x: 2, y: 2, z: 4, core: 2. Of those that a mesh axis runs over, the one named last changes fastest.
Arguments:
- tokens: bfloat16 [32, 1024, 768], P(('wide', 'narrow')), may hold values from -6 to 6
- cotangent: bfloat16 [32, 1024, 768], P(('wide', 'narrow')), may hold values from -6 to 6
- segment_ids: int32 [32, 1024], P(('wide', 'narrow')), may hold values from 0 to 3, never falling along the last dimension, each value on 1 to 512 neighbouring positions
- routes: int32 [32, 1024, 2], P(('wide', 'narrow')), may hold values from 0 to 3, all different within a row; in each aligned block of 1024 rows (0 to 1023, 1024 to 2047, ..., all dimensions but the last counted through in order) at most 640 rows name the same one
- replay: int32 [32, 1024], P(('wide', 'narrow')), may hold values 0 or 1
- gain_one: bfloat16 [768], P(('wide', 'narrow')), may hold values from 0.099609375 to 1.8984375
- shift_one: bfloat16 [768], P(('wide', 'narrow')), may hold values from -3 to 3
- w_query: bfloat16 [768, 768], P(('wide', 'narrow')), may hold values from -0.21875 to 0.21875
- b_query: bfloat16 [768], P(('wide', 'narrow')), may hold values from -3 to 3
- w_key: bfloat16 [768, 768], P(('wide', 'narrow')), may hold values from -0.21875 to 0.21875
- w_value: bfloat16 [768, 768], P(('wide', 'narrow')), may hold values from -0.21875 to 0.21875
- b_value: bfloat16 [768], P(('wide', 'narrow')), may hold values from -3 to 3
- w_out: bfloat16 [768, 768], P(('wide', 'narrow')), may hold values from -0.875 to 0.875
- b_out: bfloat16 [768], P(('wide', 'narrow')), may hold values from -3 to 3
- gain_two: bfloat16 [768], P(('wide', 'narrow')), may hold values from 0.099609375 to 1.8984375
- shift_two: bfloat16 [768], P(('wide', 'narrow')), may hold values from -3 to 3
- w_router: bfloat16 [768, 4], P(('wide', 'narrow')), may hold values from -0.4375 to 0.4375
- new_up: bfloat16 [2, 768, 3072], P(None, ('wide', 'narrow')), may hold values from -0.21875 to 0.21875
- new_up_bias: bfloat16 [2, 3072], P(None, ('wide', 'narrow')), may hold values from -3 to 3
- new_down: bfloat16 [2, 3072, 768], P(None, ('wide', 'narrow')), may hold values from -0.109375 to 0.109375
- new_down_bias: bfloat16 [2, 768], P(None, ('wide', 'narrow')), may hold values from -3 to 3
- old_up: bfloat16 [2, 768, 3072], P(None, ('wide', 'narrow')), may hold values from -0.21875 to 0.21875
- old_up_bias: bfloat16 [2, 3072], P(None, ('wide', 'narrow')), may hold values from -3 to 3
- old_down: bfloat16 [2, 3072, 768], P(None, ('wide', 'narrow')), may hold values from -0.109375 to 0.109375
- old_down_bias: bfloat16 [2, 768], P(None, ('wide', 'narrow')), may hold values from -3 to 3
Outputs:
- output: bfloat16 [32, 1024, 768], P(('wide', 'narrow'))
- grad_tokens: bfloat16 [32, 1024, 768], P(('wide', 'narrow'))
- grad_gain_one: float32 [768], P(('wide', 'narrow'))
- grad_shift_one: float32 [768], P(('wide', 'narrow'))
- grad_w_query: float32 [768, 768], P(('wide', 'narrow'))
- grad_b_query: float32 [768], P(('wide', 'narrow'))
- grad_w_key: float32 [768, 768], P(('wide', 'narrow'))
- grad_w_value: float32 [768, 768], P(('wide', 'narrow'))
- grad_b_value: float32 [768], P(('wide', 'narrow'))
- grad_w_out: float32 [768, 768], P(('wide', 'narrow'))
- grad_b_out: float32 [768], P(('wide', 'narrow'))
- grad_gain_two: float32 [768], P(('wide', 'narrow'))
- grad_shift_two: float32 [768], P(('wide', 'narrow'))
- grad_w_router: float32 [768, 4], P(('wide', 'narrow'))
- grad_new_up: float32 [2, 768, 3072], P(None, ('wide', 'narrow'))
- grad_new_up_bias: float32 [2, 3072], P(None, ('wide', 'narrow'))
- grad_new_down: float32 [2, 3072, 768], P(None, ('wide', 'narrow'))
- grad_new_down_bias: float32 [2, 768], P(None, ('wide', 'narrow'))
The draws below stay inside these ranges and needn't reach their ends.
Inputs may be any that keep to these rules, and one draw needn't show every extreme that they name: `routes`: each row names 2 different experts. Among the 1024 rows of one device, no expert is named by more than 640 rows, and in every draw some device has an expert named by exactly 640. `segment_ids`: within a sequence the numbers never fall; each document has 1 to 512 tokens, and one has exactly 512.
All inputs are finite; a program needn't handle non-finite values. No bound on the sum of `replay` on one device may be relied on, other than what follows from the above.
Results may differ from the reference program's by a relative error of at most 0.015.
Values may be sent and summed in bfloat16 or wider, within the bound.
A program may use at most 384 MiB of HBM per device.

```python
import math
import jax
import jax.numpy as jnp
import numpy as np
from jax import lax

D = 768
H = 12
HD = 64
FF = 3072
FROZEN = 2
NEW_EXP = 2
TOP = 2
L = 1024
SEGS = 4
EXPERTS = 4
TOK_DEV = 1024
CAP = 640
SEQS = 32


def touch_ends(entries, own_key, smallest, largest):
    longest = entries.shape.index(max(entries.shape))
    spots = []
    for shift in (0, 1):
        where = [jax.random.randint(jax.random.fold_in(own_key, axis), (), 0, length) for axis, length in enumerate(entries.shape)]
        where[longest] = (where[longest] + shift) % entries.shape[longest]
        spots.append(tuple(where))
    return entries.at[spots[0]].set(smallest).at[spots[1]].set(largest)


def raised(values, stream_key, source, target, shards_of, factor):
    def block_of(dim):
        return (jnp.arange(values.shape[dim]) // (values.shape[dim] // shards_of)).reshape((-1,) + (1,) * (values.ndim - 1 - dim))

    first = jax.random.permutation(stream_key, shards_of)[block_of(target)]
    other_side = (block_of(target) + shards_of // 2) % shards_of
    return jnp.where((block_of(source) == first) | (block_of(source) == other_side), factor * values, values)


def block_scale(stream_key, shape, pieces, least, largest):
    def one(axis_at, blocks):
        draws = jax.random.uniform(jax.random.fold_in(jax.random.fold_in(stream_key, 6), axis_at), (blocks,), jnp.float32, least / len(pieces), largest / len(pieces))
        return jnp.repeat(jnp.exp(draws), shape[axis_at] // blocks).reshape((-1,) + (1,) * (len(shape) - axis_at - 1))

    loudness = one(*pieces[0])
    for cut in pieces[1:]:
        loudness = loudness * one(*cut)
    return loudness


def profile(count, total, bound, lean):
    weights = [(1 << 20) // math.isqrt(standing ** lean) + 1 for standing in range(2, count + 1)]
    rest, counts = total - bound - (count - 1), [1] * (count - 1)
    while rest > 0:
        candidates = [i for i in range(count - 1) if counts[i] < bound]
        pool, remaining = sum([weights[i] for i in candidates]), rest
        for i in candidates:
            extra = min(bound - counts[i], max(1, remaining * weights[i] // pool), rest)
            counts[i] = counts[i] + extra
            rest = rest - extra
    return np.array([bound] + counts)


def uneven_parts(rng, amount, total, reach, slope):
    if amount == 2:
        one = jax.random.randint(rng, (), max(1, total - reach), min(reach, total - 1) + 1)
        return jnp.stack([one, total - one])
    sizes = jnp.asarray(profile(amount, total, reach, slope), jnp.int32)
    pairs = (amount - 1) // 2
    giver, sink = sizes[1:1 + 2 * pairs:2], sizes[2:2 + 2 * pairs:2]
    room = jnp.minimum(giver - 1, reach - sink)
    shifted = jax.random.randint(jax.random.fold_in(rng, 1), (pairs,), 0, 1 << 20) % (room + 1)
    sizes = sizes.at[1:1 + 2 * pairs:2].set(giver - shifted).at[2:2 + 2 * pairs:2].set(sink + shifted)
    return sizes[jax.random.permutation(jax.random.fold_in(rng, 2), amount)]


def assign_block(key, own, number, rows, count, top, limit, slope):
    order = jax.random.permutation(key, count)
    heavy_load, common = portions_of(count, rows * top, limit, slope, True), portions_of(count, rows * top, limit, slope, False)
    places = jnp.arange(count)

    def named(lengths, turn):
        used = int((lengths > 0).sum())
        fixed = max(1, used // 4)
        passed = fixed + (places - fixed + turn * (used - fixed)) % max(1, count - fixed)
        return jnp.zeros((count,), jnp.int32).at[order[jnp.where(places < fixed, places, passed)]].set(jnp.asarray(lengths, jnp.int32))

    lengths = jnp.where(number % 4 == 0, named(heavy_load, number // 4), named(common, number - number // 4 - 1))
    mixed = jax.random.permutation(jax.random.fold_in(own, 3), count)
    donor, taker = mixed[0:count // 2 * 2:2], mixed[1:count // 2 * 2:2]
    margin = jnp.minimum(lengths[donor] - 1, limit - lengths[taker]) // 2
    margin = jnp.where((donor == order[0]) | (taker == order[0]) | (lengths[taker] == 0), 0, jnp.maximum(margin, 0))
    passed = jax.random.randint(jax.random.fold_in(own, 4), (count // 2,), 0, 1 << 20) % (margin + 1)
    lengths = lengths.at[donor].add(-passed).at[taker].add(passed)
    members = jnp.searchsorted(jnp.cumsum(lengths), jnp.arange(rows * top), side="right").astype(jnp.int32)
    table = members.reshape(top, rows).T
    table = table[jax.random.permutation(jax.random.fold_in(own, 1), rows)]
    turn = jax.random.randint(jax.random.fold_in(own, 2), (rows, 1), 0, top)
    return jnp.take_along_axis(table, (jnp.arange(top)[None, :] + turn) % top, axis=1)


def portions_of(count, total, reach, slope, full):
    loads = [(1 << 20) // math.isqrt(standing ** slope) + 1 for standing in range(1, count + 1)]
    largest = reach if full else min(reach, max(-(-total // count), total * loads[0] // sum(loads)))
    least = 1 if total - largest >= count - 1 else 0
    counts, spare = [largest] + [least] * (count - 1), total - largest - least * (count - 1)
    while spare > 0:
        movable = [i for i in range(1, count) if counts[i] < largest] or [i for i in range(1, count) if counts[i] < reach]
        whole, budget = sum([loads[i] for i in movable]), spare
        for i in movable:
            more = min(reach - counts[i], max(1, budget * loads[i] // whole), spare)
            counts[i] = counts[i] + more
            spare = spare - more
    return np.array(counts)


def centred(stream_key, dims, width, limit, shards=(), kind=jnp.bfloat16):
    values = jax.random.normal(stream_key, dims, jnp.float32) * width
    if len(shards) > 0:
        values = block_scale(stream_key, dims, shards, -0.22, 0.18) * values
    return jnp.clip(values, min=-limit, max=limit).astype(kind)


def gaussian_with(key, extent, width, most, cuts, heavy, kind=jnp.bfloat16):
    values = width * jax.random.normal(key, extent, jnp.float32)
    if cuts:
        values = values * block_scale(key, extent, cuts, -0.22, 0.18)
    return jnp.clip(raised(values, jax.random.fold_in(key, 3), *heavy), -most, most).astype(kind)


def setup_inputs(seed: int = 0) -> dict:
    key_of = jax.random.split(jax.random.key(seed), 26)
    tokens = centred(key_of[0], (SEQS, L, D), 1.0, 6.0, ((0, 32),))
    cotangent = gaussian_with(key_of[1], (SEQS, L, D), 1.0, 6.0, ((0, 32),), (0, 2, 32, 2.75))
    segment_ids = jax.vmap(lambda own: jnp.searchsorted(jnp.cumsum(uneven_parts(own, SEGS, L, L // 2, 1)), jnp.arange(L), side="right"))(jax.random.split(key_of[2], SEQS)).reshape((SEQS, L)).astype(jnp.int32)
    routes_keys = jax.random.split(jax.random.fold_in(key_of[3], 1), SEQS * L // TOK_DEV)
    routes_turns = jax.random.permutation(jax.random.fold_in(key_of[3], 3), SEQS * L // TOK_DEV)
    routes = jax.vmap(lambda own, number: assign_block(jax.random.fold_in(key_of[3], 2), own, number, TOK_DEV, EXPERTS, TOP, CAP, 1))(routes_keys, routes_turns).reshape((SEQS, L, TOP))
    replay = touch_ends((jax.random.randint(key_of[4], (SEQS, L), 0, 4) < 1).astype(jnp.int32), jax.random.fold_in(key_of[4], 1), 0, 1)
    gain_one = jnp.clip(1.0 + 0.18 * jax.random.normal(key_of[5], (D,), jnp.float32), 0.099609375, 1.8984375).astype(jnp.bfloat16)
    shift_one = centred(key_of[6], (D,), 0.5, 3.0, ((0, 32),))
    w_query = centred(key_of[7], (D, D), D ** -0.5, 0.21875, ((0, 32),))
    b_query = centred(key_of[8], (D,), 0.5, 3.0, ((0, 32),))
    w_key = centred(key_of[9], (D, D), D ** -0.5, 0.21875, ((0, 32),))
    w_value = centred(key_of[10], (D, D), D ** -0.5, 0.21875, ((0, 32),))
    b_value = centred(key_of[11], (D,), 0.5, 3.0, ((0, 32),))
    w_out = centred(key_of[12], (D, D), (D // 16) ** -0.5, 0.875, ((0, 32),))
    b_out = centred(key_of[13], (D,), 0.5, 3.0, ((0, 32),))
    gain_two = jnp.clip(1.0 + 0.18 * jax.random.normal(key_of[14], (D,), jnp.float32), 0.099609375, 1.8984375).astype(jnp.bfloat16)
    shift_two = centred(key_of[15], (D,), 0.5, 3.0, ((0, 32),))
    w_router = centred(key_of[16], (D, EXPERTS), (D // 4) ** -0.5, 0.4375, ((0, 32),))
    new_up = centred(key_of[17], (NEW_EXP, D, FF), D ** -0.5, 0.21875, ((1, 32),))
    new_up_bias = centred(key_of[18], (NEW_EXP, FF), 0.5, 3.0, ((1, 32),))
    new_down = centred(key_of[19], (NEW_EXP, FF, D), FF ** -0.5, 0.109375, ((1, 32),))
    new_down_bias = centred(key_of[20], (NEW_EXP, D), 0.5, 3.0, ((1, 32),))
    old_up = centred(key_of[21], (FROZEN, D, FF), D ** -0.5, 0.21875, ((1, 32),))
    old_up_bias = centred(key_of[22], (FROZEN, FF), 0.5, 3.0, ((1, 32),))
    old_down = centred(key_of[23], (FROZEN, FF, D), FF ** -0.5, 0.109375, ((1, 32),))
    old_down_bias = centred(key_of[24], (FROZEN, D), 0.5, 3.0, ((1, 32),))
    return {"tokens": tokens, "cotangent": cotangent, "segment_ids": segment_ids, "routes": routes, "replay": replay, "gain_one": gain_one, "shift_one": shift_one, "w_query": w_query, "b_query": b_query, "w_key": w_key, "w_value": w_value, "b_value": b_value, "w_out": w_out, "b_out": b_out, "gain_two": gain_two, "shift_two": shift_two, "w_router": w_router, "new_up": new_up, "new_up_bias": new_up_bias, "new_down": new_down, "new_down_bias": new_down_bias, "old_up": old_up, "old_up_bias": old_up_bias, "old_down": old_down, "old_down_bias": old_down_bias}


@jax.custom_vjp
def low(v):
    return lax.optimization_barrier(v.astype(jnp.bfloat16)).astype(jnp.float32)

@jax.custom_vjp
def low_back(v):
    return v

def low_keep(v):
    return (low(v), None)

def low_pass(kept, grad):
    return (grad,)

def back_keep(v):
    return (v, None)

def back_low(kept, grad):
    return (low(grad),)
low.defvjp(low_keep, low_pass)
low_back.defvjp(back_keep, back_low)
epsilon = 1e-05
masked_score = -1e+30
batch_seqs = 4
highest = lax.Precision.HIGHEST

def layer_norm(inputs, gain, shift):
    center = inputs - lax.optimization_barrier(jnp.mean(inputs, axis=-1, keepdims=True))
    spread = lax.optimization_barrier(jnp.mean(center * center, axis=-1, keepdims=True))
    return center * lax.rsqrt(spread + epsilon) * gain + shift

def product(left, right):
    return jnp.matmul(left, right, precision=highest)

def route_weights(logits, route_ids, replay_rows):
    gate = jax.nn.softmax(logits, axis=-1)
    picked = jnp.take_along_axis(gate, route_ids, axis=-1)
    shares = picked / lax.optimization_barrier(jnp.sum(picked, axis=-1, keepdims=True))
    trained = (route_ids >= FROZEN).astype(shares.dtype)
    return shares * (1.0 - replay_rows[..., None].astype(shares.dtype) * trained)

def forward_group(params, frozen, inputs, documents, route_ids, replay_rows):
    gain_one, shift_one, w_query, b_query, w_key, w_value, b_value, w_out, b_out, gain_two, shift_two, w_router, new_up, new_up_bias, new_down, new_down_bias = params
    old_up, old_up_bias, old_down, old_down_bias = frozen
    groups = inputs.shape[0]
    normed = low_back(low(layer_norm(inputs, gain_one, shift_one)))
    query = low_back(low(product(normed, w_query) + b_query)).reshape(groups, L, H, HD)
    keys = low_back(low(product(normed, w_key))).reshape(groups, L, H, HD)
    values = low_back(low(product(normed, w_value) + b_value)).reshape(groups, L, H, HD)
    scores = jnp.einsum('gqhd,gkhd->ghqk', query, keys, precision=highest) * HD ** (-0.5)
    scores = low_back(scores)
    places = jnp.arange(L, dtype=jnp.int32)
    allowed = (documents[:, None, :, None] == documents[:, None, None, :]) & (places[:, None] >= places[None, :])[None, None]
    scores = jnp.where(allowed, scores, masked_score)
    weights = low(jax.nn.softmax(scores, axis=-1))
    mixed = jnp.einsum('ghqk,gkhd->gqhd', weights, values, precision=highest).reshape(groups, L, D)
    mixed = low_back(low(mixed))
    resid = inputs + low_back(product(mixed, w_out) + b_out)
    normed_two = low_back(low(layer_norm(resid, gain_two, shift_two)))
    logits = product(normed_two, w_router)
    combine = route_weights(logits, route_ids, replay_rows)
    table = lax.optimization_barrier(jnp.sum(combine[..., None] * jax.nn.one_hot(route_ids, EXPERTS, dtype=combine.dtype), axis=-2))
    up_all = jnp.concatenate([old_up, new_up], axis=0)
    up_bias_all = jnp.concatenate([old_up_bias, new_up_bias], axis=0)
    down_all = jnp.concatenate([old_down, new_down], axis=0)
    down_bias_all = jnp.concatenate([old_down_bias, new_down_bias], axis=0)
    hidden = low_back(jnp.einsum('gld,edf->gelf', normed_two, up_all, precision=highest) + up_bias_all[None, :, None, :])
    active = low(jax.nn.gelu(hidden))
    expert_out = low_back(jnp.einsum('gelf,efd->geld', active, down_all, precision=highest) + down_bias_all[None, :, None, :])
    return resid + jnp.einsum('gle,geld->gld', table, expert_out, precision=highest)

def reference(tokens, cotangent, segment_ids, routes, replay, gain_one, shift_one, w_query, b_query, w_key, w_value, b_value, w_out, b_out, gain_two, shift_two, w_router, new_up, new_up_bias, new_down, new_down_bias, old_up, old_up_bias, old_down, old_down_bias):
    trainable = tuple((item.astype(jnp.float32) for item in (gain_one, shift_one, w_query, b_query, w_key, w_value, b_value, w_out, b_out, gain_two, shift_two, w_router, new_up, new_up_bias, new_down, new_down_bias)))
    frozen = tuple((item.astype(jnp.float32) for item in (old_up, old_up_bias, old_down, old_down_bias)))
    steps_count = SEQS // batch_seqs
    documents = segment_ids.reshape(steps_count, batch_seqs, L)
    route_ids = routes.reshape(steps_count, batch_seqs, L, TOP)
    replay_rows = replay.reshape(steps_count, batch_seqs, L)
    checked = jax.checkpoint(forward_group)

    def whole(inputs, params):

        def advance(carry, batch):
            piece, document, route_piece, replay_piece = batch
            return (carry, checked(params, frozen, piece, document, route_piece, replay_piece))
        _, result = lax.scan(advance, (), (inputs.reshape(steps_count, batch_seqs, L, D), documents, route_ids, replay_rows))
        return result.reshape(SEQS, L, D)
    result, pullback = jax.vjp(whole, tokens.astype(jnp.float32), trainable)
    grad_input, grads = pullback(cotangent.astype(jnp.float32))
    return (result.astype(jnp.bfloat16), grad_input.astype(jnp.bfloat16), grads[0], grads[1], grads[2], grads[3], grads[4], grads[5], grads[6], grads[7], grads[8], grads[9], grads[10], grads[11], grads[12], grads[13], grads[14], grads[15])
```

```python
import functools

import jax
import jax.numpy as jnp
from jax import lax
from jax.experimental import pallas as pl
from jax.experimental.pallas import tpu as pltpu
from jax.sharding import PartitionSpec as P

HD = 64
FROZEN = 2
EXPERTS = 4
CAP = 640
BLOCK = 256
LONGEST = 512
TILE = 128
AXES = ("wide", "narrow")

epsilon = 1e-05
masked_score = -1e30
f32 = jnp.float32
bf16 = jnp.bfloat16


def dot(a, b):
    return jnp.dot(a, b, preferred_element_type=f32)


def dot_nt(a, b):
    return lax.dot_general(a, b, (((1,), (1,)), ((), ())), preferred_element_type=f32)


def dot_tn(a, b):
    return lax.dot_general(a, b, (((0,), (0,)), ((), ())), preferred_element_type=f32)


def band(index):
    start = max(0, index - LONGEST // BLOCK) * BLOCK
    return start, (index + 1) * BLOCK - start


def attn_forward_kernel(q_ref, k_ref, v_ref, seg_col, seg_row, out_ref, prob_ref):
    length = q_ref.shape[0]
    first = lax.broadcasted_iota(jnp.int32, (BLOCK, 2 * HD), 1) < HD
    for index in range(length // BLOCK):
        start, size = band(index)
        rows = pl.ds(index * BLOCK, BLOCK)
        cols = pl.ds(start, size)
        place_q = lax.broadcasted_iota(jnp.int32, (BLOCK, size), 0) + (index * BLOCK - start)
        place_k = lax.broadcasted_iota(jnp.int32, (BLOCK, size), 1)
        allowed = (seg_col[rows, :] == seg_row[:, cols]) & (place_q >= place_k)
        query = q_ref[rows, :] * jnp.asarray(HD**-0.5, bf16)
        zero = jnp.zeros_like(query)
        keys = k_ref[cols, :]
        values = v_ref[cols, :]
        parts = []
        for head in range(2):
            mine = first if head == 0 else jnp.logical_not(first)
            scores = dot_nt(jnp.where(mine, query, zero), keys)
            scores = jnp.where(allowed, scores, masked_score)
            expon = jnp.exp(scores - jnp.max(scores, axis=-1, keepdims=True))
            total = jnp.sum(expon, axis=-1, keepdims=True)
            weights = (expon * (1.0 / total)).astype(bf16)
            prob_ref[head, rows, pl.ds(0, size)] = weights
            parts.append(dot(weights, values))
        out_ref[rows, :] = jnp.where(first, parts[0], parts[1]).astype(bf16)


def attn_forward(query, keys, values, seg_col, seg_row):
    length, width = query.shape
    pairs = width // (2 * HD)
    span = min(length, LONGEST + BLOCK)
    col = pl.BlockSpec((length, 2 * HD), lambda p: (0, p))
    return pl.pallas_call(
        attn_forward_kernel,
        grid=(pairs,),
        in_specs=[
            col,
            col,
            col,
            pl.BlockSpec((length, 1), lambda p: (0, 0)),
            pl.BlockSpec((1, length), lambda p: (0, 0)),
        ],
        out_specs=[col, pl.BlockSpec((2, length, span), lambda p: (p, 0, 0))],
        out_shape=[
            jax.ShapeDtypeStruct((length, width), bf16),
            jax.ShapeDtypeStruct((2 * pairs, length, span), bf16),
        ],
        compiler_params=pltpu.CompilerParams(vmem_limit_bytes=60 << 20),
        cost_estimate=pl.CostEstimate(
            flops=20 * 10**9, bytes_accessed=30 * 10**6, transcendentals=8 * 10**6
        ),
        name="attn_forward",
    )(query, keys, values, seg_col, seg_row)


def attn_backward_kernel(q_ref, k_ref, v_ref, grad_ref, prob_ref, gq_ref, gk_ref, gv_ref, gk, gv):
    length = q_ref.shape[0]
    first = lax.broadcasted_iota(jnp.int32, (BLOCK, 2 * HD), 1) < HD
    gk[...] = jnp.zeros_like(gk)
    gv[...] = jnp.zeros_like(gv)
    for index in range(length // BLOCK):
        start, size = band(index)
        rows = pl.ds(index * BLOCK, BLOCK)
        cols = pl.ds(start, size)
        query = q_ref[rows, :]
        grad = grad_ref[rows, :]
        keys = k_ref[cols, :]
        values = v_ref[cols, :]
        zero = jnp.zeros_like(query)
        parts = []
        for head in range(2):
            mine = first if head == 0 else jnp.logical_not(first)
            grad_head = jnp.where(mine, grad, zero)
            probs = prob_ref[head, rows, pl.ds(0, size)]
            grad_weights = dot_nt(grad_head, values)
            wide = probs.astype(f32)
            inner = jnp.sum(wide * grad_weights, axis=-1, keepdims=True)
            grad_scores = (wide * (grad_weights - inner)).astype(bf16)
            parts.append(dot(grad_scores, keys))
            gk[cols, :] += dot_tn(grad_scores, jnp.where(mine, query, zero))
            gv[cols, :] += dot_tn(probs, grad_head)
        gq_ref[rows, :] = (jnp.where(first, parts[0], parts[1]) * HD**-0.5).astype(bf16)
    gk_ref[...] = (gk[...] * HD**-0.5).astype(bf16)
    gv_ref[...] = gv[...].astype(bf16)


def attn_backward(query, keys, values, grad, probs):
    length, width = query.shape
    pairs = width // (2 * HD)
    span = probs.shape[-1]
    col = pl.BlockSpec((length, 2 * HD), lambda p: (0, p))
    shape = jax.ShapeDtypeStruct((length, width), bf16)
    return pl.pallas_call(
        attn_backward_kernel,
        grid=(pairs,),
        in_specs=[col, col, col, col, pl.BlockSpec((2, length, span), lambda p: (p, 0, 0))],
        out_specs=[col, col, col],
        out_shape=[shape, shape, shape],
        scratch_shapes=[pltpu.VMEM((length, 2 * HD), f32), pltpu.VMEM((length, 2 * HD), f32)],
        compiler_params=pltpu.CompilerParams(vmem_limit_bytes=60 << 20),
        cost_estimate=pl.CostEstimate(
            flops=50 * 10**9, bytes_accessed=30 * 10**6, transcendentals=0
        ),
        name="attn_backward",
    )(query, keys, values, grad, probs)


def expert_kernel(train, counts, *refs):
    inputs, outputs, scratch = refs[:9], refs[9 : 9 + (7 if train else 3)], refs[-6:]
    normed, cot, share, pos_row, pos_col, up_w, up_b, down_w, down_b = inputs
    out_ref, gx_ref, gc_ref = outputs[:3]
    rows_x, rows_g, rows_out, rows_gx, rows_act, rows_gu = scratch
    expert, chunk = pl.program_id(0), pl.program_id(1)
    length = normed.shape[0]

    @pl.when((expert == 0) & (chunk == 0))
    def _():
        out_ref[...] = jnp.zeros_like(out_ref)
        gx_ref[...] = jnp.zeros_like(gx_ref)
        rows_act[...] = jnp.zeros_like(rows_act)
        rows_gu[...] = jnp.zeros_like(rows_gu)

    @pl.when(chunk == 0)
    def _():
        slots = lax.broadcasted_iota(jnp.int32, (CAP, length), 0)
        select = (slots == pos_row[0]).astype(bf16)
        rows_x[...] = dot(select, normed[...]).astype(bf16)
        scaled = (cot[...].astype(f32) * share[0]).astype(bf16)
        grads = dot(select, scaled)
        rows_g[...] = grads.astype(bf16)
        rows_out[...] = jnp.broadcast_to(down_b[0].astype(f32), rows_out.shape)
        rows_gx[...] = jnp.zeros_like(rows_gx)
        if train:
            outputs[6][0] = jnp.sum(grads, axis=0, keepdims=True)

    bias = up_b[0].astype(f32)

    def tile(step, total):
        here = pl.ds(pl.multiple_of(step * TILE, TILE), TILE)
        up = dot(rows_x[here, :], up_w[0, 0]) + bias
        square = up * up
        bent = jnp.tanh(0.7978845608028654 * up * (1.0 + 0.044715 * square))
        half = 0.5 + 0.5 * bent
        active = (up * half).astype(bf16)
        slope = half + (0.5 * 0.7978845608028654) * up * (1.0 - bent * bent) * (
            1.0 + (3 * 0.044715) * square
        )
        rows_out[here, :] += dot(active, down_w[0])
        grad_up = (dot_nt(rows_g[here, :], down_w[0]) * slope).astype(bf16)
        rows_gx[here, :] += dot_nt(grad_up, up_w[0, 0])
        if train:
            rows_act[here, :] = active
            rows_gu[here, :] = grad_up
            return total + jnp.sum(grad_up.astype(f32), axis=0, keepdims=True)
        return total

    tiles = (counts[expert] + (TILE - 1)) // TILE
    total = lax.fori_loop(0, tiles, tile, jnp.zeros((1, up_b.shape[-1]), f32))
    if train:
        outputs[4][0] = total
        outputs[3][0, 0] = dot_tn(rows_x[...], rows_gu[...]).astype(bf16)
        outputs[5][0] = dot_tn(rows_act[...], rows_g[...]).astype(bf16)

    @pl.when(chunk == pl.num_programs(1) - 1)
    def _():
        slots = lax.broadcasted_iota(jnp.int32, (length, CAP), 1)
        select = (slots == pos_col[0]).astype(bf16)
        expert_out = dot(select, rows_out[...].astype(bf16))
        gc_ref[0] = jnp.sum(cot[...].astype(f32) * expert_out, axis=-1, keepdims=True)
        out_ref[...] += share[0] * expert_out
        gx_ref[...] += dot(select, rows_gx[...].astype(bf16))


def experts(train, counts, normed, cot, share, pos_row, pos_col, up_w, up_b, down_w, down_b):
    length, width = normed.shape
    number, chunks = up_w.shape[:2]
    part = up_w.shape[-1]
    whole = pl.BlockSpec((length, width), lambda e, j, c: (0, 0))
    column = pl.BlockSpec((1, length, 1), lambda e, j, c: (e, 0, 0))
    up_spec = pl.BlockSpec((1, 1, width, part), lambda e, j, c: (e, j, 0, 0))
    down_spec = pl.BlockSpec((1, part, width), lambda e, j, c: (e, j, 0))
    bias_spec = pl.BlockSpec((1, 1, part), lambda e, j, c: (e, 0, j))
    last_spec = pl.BlockSpec((1, 1, width), lambda e, j, c: (e, 0, 0))
    out_specs = [whole, whole, column]
    out_shape = [
        jax.ShapeDtypeStruct((length, width), f32),
        jax.ShapeDtypeStruct((length, width), f32),
        jax.ShapeDtypeStruct((number, length, 1), f32),
    ]
    if train:
        out_specs += [up_spec, bias_spec, down_spec, last_spec]
        out_shape += [
            jax.ShapeDtypeStruct(up_w.shape, bf16),
            jax.ShapeDtypeStruct(up_b.shape, f32),
            jax.ShapeDtypeStruct(down_w.shape, bf16),
            jax.ShapeDtypeStruct(down_b.shape, f32),
        ]
    return pl.pallas_call(
        functools.partial(expert_kernel, train),
        grid_spec=pltpu.PrefetchScalarGridSpec(
            num_scalar_prefetch=1,
            grid=(number, chunks),
            in_specs=[
                whole,
                whole,
                column,
                pl.BlockSpec((1, 1, length), lambda e, j, c: (e, 0, 0)),
                column,
                up_spec,
                bias_spec,
                down_spec,
                last_spec,
            ],
            out_specs=out_specs,
            scratch_shapes=[
                pltpu.VMEM((CAP, width), bf16),
                pltpu.VMEM((CAP, width), bf16),
                pltpu.VMEM((CAP, width), f32),
                pltpu.VMEM((CAP, width), f32),
                pltpu.VMEM((CAP, part), bf16),
                pltpu.VMEM((CAP, part), bf16),
            ],
        ),
        out_shape=out_shape,
        compiler_params=pltpu.CompilerParams(vmem_limit_bytes=60 << 20),
        cost_estimate=pl.CostEstimate(
            flops=(45 if train else 32) * 10**9,
            bytes_accessed=40 * 10**6,
            transcendentals=4 * 10**6,
        ),
        name="experts_new" if train else "experts_old",
    )(counts, normed, cot, share, pos_row, pos_col, up_w, up_b, down_w, down_b)


def normalize(inputs):
    center = inputs - jnp.mean(inputs, axis=-1, keepdims=True)
    spread = jnp.mean(center * center, axis=-1, keepdims=True)
    scale = lax.rsqrt(spread + epsilon)
    return center * scale, scale


def normalize_back(unit, scale, grad):
    average = jnp.mean(grad, axis=-1, keepdims=True)
    along = jnp.mean(grad * unit, axis=-1, keepdims=True)
    return scale * (grad - average - unit * along)


def pack_experts(up, down):
    number, rows, width = up.shape[0], up.shape[1], down.shape[2]
    chunks = up.shape[2] // width
    tall = up.reshape(number, rows, chunks, width).transpose(0, 2, 1, 3)
    tall = tall.reshape(number, chunks * rows, width)
    return jnp.concatenate([tall, down], axis=1).reshape(-1, width)


def unpack_experts(gathered, number, rows):
    count, width = gathered.shape[0], gathered.shape[2]
    both = gathered.reshape(count, number, -1, width)
    tall = both.shape[2] // 2
    chunks = tall // rows
    up = both[:, :, :tall].reshape(count, number, chunks, rows, width)
    up = up.transpose(1, 2, 0, 3, 4).reshape(number, chunks, count * rows, width)
    down = both[:, :, tall:].transpose(1, 0, 2, 3).reshape(number, count * tall, width)
    return up, down


def local(
    tokens,
    cotangent,
    segment_ids,
    routes,
    replay,
    gain_one,
    shift_one,
    w_query,
    b_query,
    w_key,
    w_value,
    b_value,
    w_out,
    b_out,
    gain_two,
    shift_two,
    w_router,
    new_up,
    new_up_bias,
    new_down,
    new_down_bias,
    old_up,
    old_up_bias,
    old_down,
    old_down_bias,
):
    seqs_here, length, width = tokens.shape
    part = w_query.shape[0]
    count = width // part
    hidden = new_up.shape[-1]
    new_count = new_up.shape[0]

    small = [gain_one, shift_one, b_query, b_value, b_out, gain_two, shift_two]
    small += [w_router, new_up_bias, old_up_bias, new_down_bias, old_down_bias]
    vector = jnp.concatenate([item.reshape(-1) for item in small])
    sizes = [item.size for item in small]
    vector = jnp.pad(vector, (0, 8 * width - vector.size)).reshape(8, width)
    first_pack = jnp.concatenate([w_query, w_key, w_value, w_out, vector], axis=0)
    new_pack = pack_experts(new_up, new_down)
    old_pack = pack_experts(old_up, old_down)
    first = lax.all_gather(first_pack, AXES, axis=0)
    new_pack, first = lax.optimization_barrier((new_pack, first))
    new_all = lax.all_gather(new_pack, AXES, axis=0)

    full = first[:, : 4 * part].reshape(count, 4, part, width).transpose(1, 0, 2, 3)
    full = full.reshape(4, width, width)
    full_query, full_key, full_value, full_out = full[0], full[1], full[2], full[3]
    flat_small = first[:, 4 * part]
    marks = [0]
    for size in sizes:
        marks.append(marks[-1] + size)

    def vector_of(index):
        return flat_small[:, marks[index] : marks[index + 1]]

    seven = flat_small[:, : 7 * part].reshape(count, 7, part).transpose(1, 0, 2)
    seven = seven.reshape(7, width).astype(f32)
    gain_first, shift_first, bias_q, bias_v, bias_o, gain_second, shift_second = seven
    router = vector_of(7).reshape(width, EXPERTS)
    biases = []
    for index in (8, 9, 10, 11):
        item = vector_of(index).reshape(count, new_count, -1).transpose(1, 0, 2)
        biases.append(item.reshape(new_count, 1, -1))
    new_up_b, old_up_b, new_down_b, old_down_b = biases

    flat = tokens.reshape(length, width).astype(f32)
    cot = cotangent.reshape(length, width)
    segments = segment_ids.reshape(length)
    route_flat = routes.reshape(length, -1)
    member = jnp.any(
        route_flat[:, :, None] == jnp.arange(EXPERTS, dtype=jnp.int32)[None, None, :], axis=1
    )
    member_int = member.astype(jnp.int32)
    running = jnp.cumsum(member_int, axis=0)
    position = jnp.where(member, running - 1, -1)
    pos_row = position.T[:, None, :]
    pos_col = position.T[:, :, None]
    counts = running[-1]

    unit_one, scale_one = normalize(flat)
    normed = (unit_one * gain_first + shift_first).astype(bf16)
    query = (dot(normed, full_query) + bias_q).astype(bf16)
    keys = dot(normed, full_key).astype(bf16)
    values = (dot(normed, full_value) + bias_v).astype(bf16)
    mixed, probs = attn_forward(query, keys, values, segments[:, None], segments[None, :])
    resid = flat + dot(mixed, full_out) + bias_o
    unit_two, scale_two = normalize(resid)
    normed_two = (unit_two * gain_second + shift_second).astype(bf16)
    logits = dot(normed_two, router)
    trained = (jnp.arange(EXPERTS) >= FROZEN).astype(f32)
    keep = 1.0 - replay.reshape(length, 1).astype(f32) * trained

    def gate_map(values_in):
        gate = jax.nn.softmax(values_in, axis=-1)
        picked = jnp.where(member, gate, 0.0)
        return picked / jnp.sum(picked, axis=-1, keepdims=True) * keep

    share, gate_back = jax.vjp(gate_map, logits)
    share_cols = share.T[:, :, None]

    old_pack, new_all = lax.optimization_barrier((old_pack, new_all))
    old_all = lax.all_gather(old_pack, AXES, axis=0)
    new_up_w, new_down_w = unpack_experts(new_all, new_count, part)
    got = experts(
        True,
        counts[FROZEN:],
        normed_two,
        cot,
        share_cols[FROZEN:],
        pos_row[FROZEN:],
        pos_col[FROZEN:],
        new_up_w,
        new_up_b,
        new_down_w,
        new_down_b,
    )
    out_new, gx_new, gc_new, grad_up, grad_up_b, grad_down, grad_down_b = got
    chunks = grad_up.shape[1]
    packed_up = grad_up.reshape(new_count, chunks, count, part, width).transpose(2, 0, 1, 3, 4)
    packed_up = packed_up.reshape(count, new_count, chunks * part, width)
    packed_down = grad_down.reshape(new_count, count, -1, width).transpose(1, 0, 2, 3)
    packed = jnp.concatenate([packed_up, packed_down], axis=2).reshape(-1, width)
    summed_new = lax.psum_scatter(packed, AXES, scatter_dimension=0, tiled=True)
    summed_new = summed_new.reshape(new_count, 2, -1, width).astype(f32)
    sum_up = summed_new[:, 0].reshape(new_count, chunks, part, width).transpose(0, 2, 1, 3)
    sum_up = sum_up.reshape(new_count, part, hidden)
    sum_down = summed_new[:, 1]

    old_up_w, old_down_w = unpack_experts(old_all, new_count, part)
    out_old, gx_old, gc_old = experts(
        False,
        counts[:FROZEN],
        normed_two,
        cot,
        share_cols[:FROZEN],
        pos_row[:FROZEN],
        pos_col[:FROZEN],
        old_up_w,
        old_up_b,
        old_down_w,
        old_down_b,
    )
    result = (resid + out_new + out_old).astype(bf16)
    grad_share = jnp.concatenate([gc_old, gc_new], axis=0)[:, :, 0].T
    grad_logits = gate_back(grad_share)[0]
    grad_router = lax.dot_general(
        normed_two.astype(f32),
        grad_logits,
        (((0,), (0,)), ((), ())),
        precision=lax.Precision.HIGHEST,
        preferred_element_type=f32,
    )
    grad_two = gx_new + gx_old
    for expert in range(EXPERTS):
        grad_two = grad_two + grad_logits[:, expert : expert + 1] * router[:, expert].astype(f32)
    grad_two = grad_two.astype(bf16).astype(f32)
    grad_gain_two = jnp.sum(grad_two * unit_two, axis=0)
    grad_shift_two = jnp.sum(grad_two, axis=0)
    grad_resid = cot.astype(f32) + normalize_back(unit_two, scale_two, grad_two * gain_second)
    grad_attn = grad_resid.astype(bf16)
    grad_w_out = dot_tn(mixed, grad_attn)
    grad_b_out = jnp.sum(grad_attn.astype(f32), axis=0)
    grad_mixed = dot_nt(grad_attn, full_out).astype(bf16)
    grad_q, grad_k, grad_v = attn_backward(query, keys, values, grad_mixed, probs)
    grad_w_query = dot_tn(normed, grad_q)
    grad_w_key = dot_tn(normed, grad_k)
    grad_w_value = dot_tn(normed, grad_v)
    grad_b_query = jnp.sum(grad_q.astype(f32), axis=0)
    grad_b_value = jnp.sum(grad_v.astype(f32), axis=0)
    grad_one = dot_nt(grad_q, full_query) + dot_nt(grad_k, full_key) + dot_nt(grad_v, full_value)
    grad_one = grad_one.astype(bf16).astype(f32)
    grad_gain_one = jnp.sum(grad_one * unit_one, axis=0)
    grad_shift_one = jnp.sum(grad_one, axis=0)
    grad_input = grad_resid + normalize_back(unit_one, scale_one, grad_one * gain_first)

    pieces = [
        item.reshape(count, part, width).astype(bf16)
        for item in (grad_w_query, grad_w_key, grad_w_value, grad_w_out)
    ]
    vectors = [grad_gain_one, grad_shift_one, grad_b_query, grad_b_value, grad_b_out]
    vectors += [grad_gain_two, grad_shift_two, grad_router]
    rows = [item.reshape(count, -1) for item in vectors]
    for item in (grad_up_b, grad_down_b):
        rows.append(item.reshape(new_count, count, -1).transpose(1, 0, 2).reshape(count, -1))
    lengths = [item.shape[1] for item in rows]
    row = jnp.concatenate(rows, axis=1).astype(bf16)
    row = jnp.pad(row, ((0, 0), (0, 8 * width - row.shape[1]))).reshape(count, 8, width)
    last = jnp.concatenate(pieces + [row], axis=1).reshape(-1, width)
    summed = lax.psum_scatter(last, AXES, scatter_dimension=0, tiled=True).astype(f32)
    sums = [summed[index * part : (index + 1) * part] for index in range(4)]
    tail = summed[4 * part]
    found = []
    at = 0
    for size in lengths:
        found.append(tail[at : at + size])
        at += size
    return (
        result.reshape(seqs_here, length, width),
        grad_input.astype(bf16).reshape(seqs_here, length, width),
        found[0],
        found[1],
        sums[0],
        found[2],
        sums[1],
        sums[2],
        found[3],
        sums[3],
        found[4],
        found[5],
        found[6],
        found[7].reshape(part, EXPERTS),
        sum_up,
        found[8].reshape(new_count, -1),
        sum_down,
        found[9].reshape(new_count, -1),
    )


def solution(mesh):
    axes = AXES
    rows3 = P(axes, None, None)
    rows2 = P(axes, None)
    rows1 = P(axes)
    mid3 = P(None, axes, None)
    mid2 = P(None, axes)
    placed = (rows3, rows3, rows2, rows3, rows2)
    placed += (rows1, rows1, rows2, rows1, rows2, rows2, rows1, rows2, rows1, rows1, rows1, rows2)
    placed += (mid3, mid2) * 4
    outs = (rows3, rows3, rows1, rows1, rows2, rows1, rows2, rows2, rows1, rows2, rows1)
    outs += (rows1, rows1, rows2, mid3, mid2, mid3, mid2)
    return jax.shard_map(local, mesh=mesh, in_specs=placed, out_specs=outs, check_vma=False)
```

```python
import functools

import jax
import jax.numpy as jnp
from jax import lax
from jax.experimental import pallas as pl
from jax.experimental.pallas import tpu as pltpu
from jax.sharding import PartitionSpec as P

HD = 64
FROZEN = 2
EXPERTS = 4
CAP = 640
BLOCK = 256
LONGEST = 512
AXES = ("wide", "narrow")

epsilon = 1e-05
masked_score = -1e30
f32 = jnp.float32
bf16 = jnp.bfloat16


def dot(a, b):
    return jnp.dot(a, b, preferred_element_type=f32)


def dot_nt(a, b):
    return lax.dot_general(a, b, (((1,), (1,)), ((), ())), preferred_element_type=f32)


def dot_tn(a, b):
    return lax.dot_general(a, b, (((0,), (0,)), ((), ())), preferred_element_type=f32)


def band(index):
    start = max(0, index - LONGEST // BLOCK) * BLOCK
    return start, (index + 1) * BLOCK - start


def attn_forward_kernel(q_ref, k_ref, v_ref, seg_col, seg_row, out_ref, prob_ref):
    length = q_ref.shape[0]
    first = lax.broadcasted_iota(jnp.int32, (BLOCK, 2 * HD), 1) < HD
    for index in range(length // BLOCK):
        start, size = band(index)
        rows = pl.ds(index * BLOCK, BLOCK)
        cols = pl.ds(start, size)
        place_q = lax.broadcasted_iota(jnp.int32, (BLOCK, size), 0) + (index * BLOCK - start)
        place_k = lax.broadcasted_iota(jnp.int32, (BLOCK, size), 1)
        allowed = (seg_col[rows, :] == seg_row[:, cols]) & (place_q >= place_k)
        query = q_ref[rows, :] * jnp.asarray(HD**-0.5, bf16)
        zero = jnp.zeros_like(query)
        keys = k_ref[cols, :]
        values = v_ref[cols, :]
        parts = []
        for head in range(2):
            mine = first if head == 0 else jnp.logical_not(first)
            scores = dot_nt(jnp.where(mine, query, zero), keys)
            scores = jnp.where(allowed, scores, masked_score)
            expon = jnp.exp(scores - jnp.max(scores, axis=-1, keepdims=True))
            total = jnp.sum(expon, axis=-1, keepdims=True)
            weights = (expon * (1.0 / total)).astype(bf16)
            prob_ref[head, rows, pl.ds(0, size)] = weights
            parts.append(dot(weights, values))
        out_ref[rows, :] = jnp.where(first, parts[0], parts[1]).astype(bf16)


def attn_forward(query, keys, values, seg_col, seg_row):
    length, width = query.shape
    pairs = width // (2 * HD)
    span = min(length, LONGEST + BLOCK)
    col = pl.BlockSpec((length, 2 * HD), lambda p: (0, p))
    return pl.pallas_call(
        attn_forward_kernel,
        grid=(pairs,),
        in_specs=[
            col,
            col,
            col,
            pl.BlockSpec((length, 1), lambda p: (0, 0)),
            pl.BlockSpec((1, length), lambda p: (0, 0)),
        ],
        out_specs=[col, pl.BlockSpec((2, length, span), lambda p: (p, 0, 0))],
        out_shape=[
            jax.ShapeDtypeStruct((length, width), bf16),
            jax.ShapeDtypeStruct((2 * pairs, length, span), bf16),
        ],
        compiler_params=pltpu.CompilerParams(vmem_limit_bytes=60 << 20),
        cost_estimate=pl.CostEstimate(
            flops=20 * 10**9, bytes_accessed=30 * 10**6, transcendentals=8 * 10**6
        ),
        name="attn_forward",
    )(query, keys, values, seg_col, seg_row)


def attn_backward_kernel(q_ref, k_ref, v_ref, grad_ref, prob_ref, gq_ref, gk_ref, gv_ref, gk, gv):
    length = q_ref.shape[0]
    first = lax.broadcasted_iota(jnp.int32, (BLOCK, 2 * HD), 1) < HD
    gk[...] = jnp.zeros_like(gk)
    gv[...] = jnp.zeros_like(gv)
    for index in range(length // BLOCK):
        start, size = band(index)
        rows = pl.ds(index * BLOCK, BLOCK)
        cols = pl.ds(start, size)
        query = q_ref[rows, :]
        grad = grad_ref[rows, :]
        keys = k_ref[cols, :]
        values = v_ref[cols, :]
        zero = jnp.zeros_like(query)
        parts = []
        for head in range(2):
            mine = first if head == 0 else jnp.logical_not(first)
            grad_head = jnp.where(mine, grad, zero)
            probs = prob_ref[head, rows, pl.ds(0, size)]
            grad_weights = dot_nt(grad_head, values)
            wide = probs.astype(f32)
            inner = jnp.sum(wide * grad_weights, axis=-1, keepdims=True)
            grad_scores = (wide * (grad_weights - inner)).astype(bf16)
            parts.append(dot(grad_scores, keys))
            gk[cols, :] += dot_tn(grad_scores, jnp.where(mine, query, zero))
            gv[cols, :] += dot_tn(probs, grad_head)
        gq_ref[rows, :] = (jnp.where(first, parts[0], parts[1]) * HD**-0.5).astype(bf16)
    gk_ref[...] = (gk[...] * HD**-0.5).astype(bf16)
    gv_ref[...] = gv[...].astype(bf16)


def attn_backward(query, keys, values, grad, probs):
    length, width = query.shape
    pairs = width // (2 * HD)
    span = probs.shape[-1]
    col = pl.BlockSpec((length, 2 * HD), lambda p: (0, p))
    shape = jax.ShapeDtypeStruct((length, width), bf16)
    return pl.pallas_call(
        attn_backward_kernel,
        grid=(pairs,),
        in_specs=[col, col, col, col, pl.BlockSpec((2, length, span), lambda p: (p, 0, 0))],
        out_specs=[col, col, col],
        out_shape=[shape, shape, shape],
        scratch_shapes=[pltpu.VMEM((length, 2 * HD), f32), pltpu.VMEM((length, 2 * HD), f32)],
        compiler_params=pltpu.CompilerParams(vmem_limit_bytes=60 << 20),
        cost_estimate=pl.CostEstimate(
            flops=50 * 10**9, bytes_accessed=30 * 10**6, transcendentals=0
        ),
        name="attn_backward",
    )(query, keys, values, grad, probs)


def expert_kernel(train, chunks, *refs):
    inputs, outputs = refs[:9], refs[9 : 9 + (6 if train else 3)]
    scratch = refs[9 + len(outputs) :]
    normed, cot, share, pos_row, pos_col, up_block, up_b, down_block, down_b = inputs
    out_ref, gx_ref, gc_ref = outputs[:3]
    rows_x, rows_g, rows_out, rows_gx = scratch[:4]
    expert, chunk = pl.program_id(0), pl.program_id(1)
    last = chunks - 1
    length, width = normed.shape
    wide = up_block.shape[-1]
    up_w = up_block.reshape(width, wide)
    down_w = down_block.reshape(wide, width)

    if train:
        pack_ref = outputs[5]
        up_out, down_out, sems = scratch[4:]
        part = up_out.shape[1]
        group, tall = down_out.shape[:2]
        split = tall == (last + 1) * part

        def copies(which_expert, which_chunk):
            base = which_expert * (2 * (last + 1) * part)
            up_at = pl.multiple_of(base + which_chunk * part, 8)
            down_at = base + (last + 1) * part + (0 if split else which_chunk * tall)
            down_at = pl.multiple_of(down_at, 8)
            first = which_chunk * group if split else 0
            return (
                pltpu.make_async_copy(up_out, pack_ref.at[:, pl.ds(up_at, part), :], sems.at[0]),
                pltpu.make_async_copy(
                    down_out, pack_ref.at[pl.ds(first, group), pl.ds(down_at, tall), :], sems.at[1]
                ),
            )

    @pl.when((expert == 0) & (chunk == 0))
    def _():
        out_ref[...] = jnp.zeros_like(out_ref)
        gx_ref[...] = jnp.zeros_like(gx_ref)

    @pl.when(chunk == 0)
    def _():
        slots = lax.broadcasted_iota(jnp.int32, (CAP, length), 0)
        select = (slots == pos_row[0]).astype(bf16)
        rows_x[...] = dot(select, normed[...]).astype(bf16)
        scaled = (cot[...].astype(f32) * share[0]).astype(bf16)
        grads = dot(select, scaled)
        rows_g[...] = grads.astype(bf16)
        rows_out[...] = jnp.broadcast_to(down_b[0].astype(f32), rows_out.shape)
        rows_gx[...] = jnp.zeros_like(rows_gx)
        if train:
            outputs[4][0] = jnp.sum(grads, axis=0, keepdims=True)

    bias = up_b[0].astype(f32)

    up = dot(rows_x[...], up_w[...]) + bias
    back = dot_nt(rows_g[...], down_w[...])
    square = up * up
    bent = jnp.tanh(up * (0.7978845608028654 + (0.7978845608028654 * 0.044715) * square))
    half = 0.5 + 0.5 * bent
    active = (up * half).astype(bf16)
    slope = half + up * (half - half * bent) * (
        0.7978845608028654 + (3 * 0.044715 * 0.7978845608028654) * square
    )
    grad_up = (back * slope).astype(bf16)
    rows_out[...] += dot(active, down_w[...])
    rows_gx[...] += dot_nt(grad_up, up_w[...])
    if train:
        outputs[3][0] = jnp.sum(grad_up.astype(f32), axis=0, keepdims=True)
        previous = jnp.maximum(expert * (last + 1) + chunk - 1, 0)

        @pl.when((expert > 0) | (chunk > 0))
        def _():
            for copy in copies(previous // (last + 1), lax.rem(previous, last + 1)):
                copy.wait()

        up_out.reshape(width, wide)[...] = dot_tn(rows_x[...], grad_up).astype(bf16)
        down_out.reshape(wide, width)[...] = dot_tn(active, rows_g[...]).astype(bf16)
        for copy in copies(expert, chunk):
            copy.start()

        @pl.when((expert == pl.num_programs(0) - 1) & (chunk == last))
        def _():
            for copy in copies(expert, chunk):
                copy.wait()

    @pl.when(chunk == last)
    def _():
        slots = lax.broadcasted_iota(jnp.int32, (length, CAP), 1)
        select = (slots == pos_col[0]).astype(bf16)
        expert_out = dot(select, rows_out[...].astype(bf16))
        gc_ref[0] = jnp.sum(cot[...].astype(f32) * expert_out, axis=-1, keepdims=True)
        out_ref[...] += share[0] * expert_out
        gx_ref[...] += dot(select, rows_gx[...].astype(bf16))


def experts(train, normed, cot, share, pos_row, pos_col, up_w, down_w, up_b, down_b):
    length, width = normed.shape
    number, hidden = up_b.shape[0], up_b.shape[2]
    chunks = hidden // width
    whole = pl.BlockSpec((length, width), lambda e, j: (0, 0))
    column = pl.BlockSpec((1, length, 1), lambda e, j: (e, 0, 0))
    up_spec = pl.BlockSpec((width // up_w[1], up_w[1], width), up_w[2])
    down_spec = pl.BlockSpec((width // down_w[1], down_w[1], width), down_w[2])
    bias_spec = pl.BlockSpec((1, 1, width), lambda e, j: (e, 0, j))
    last_spec = pl.BlockSpec((1, 1, width), lambda e, j: (e, 0, 0))
    out_specs = [whole, whole, column]
    out_shape = [
        jax.ShapeDtypeStruct((length, width), f32),
        jax.ShapeDtypeStruct((length, width), f32),
        jax.ShapeDtypeStruct((number, length, 1), f32),
    ]
    scratch = [
        pltpu.VMEM((CAP, width), bf16),
        pltpu.VMEM((CAP, width), bf16),
        pltpu.VMEM((CAP, width), f32),
        pltpu.VMEM((CAP, width), f32),
    ]
    if train:
        part, tall = up_w[1], down_w[1]
        out_specs += [bias_spec, last_spec, pl.BlockSpec(memory_space=pl.ANY)]
        out_shape += [
            jax.ShapeDtypeStruct(up_b.shape, f32),
            jax.ShapeDtypeStruct(down_b.shape, f32),
            jax.ShapeDtypeStruct((width // part, number * 2 * chunks * part, width), bf16),
        ]
        scratch += [
            pltpu.VMEM((width // part, part, width), bf16),
            pltpu.VMEM((width // tall, tall, width), bf16),
            pltpu.SemaphoreType.DMA((2,)),
        ]
    return pl.pallas_call(
        functools.partial(expert_kernel, train, chunks),
        grid_spec=pltpu.PrefetchScalarGridSpec(
            num_scalar_prefetch=0,
            grid=(number, chunks),
            in_specs=[
                whole,
                whole,
                column,
                pl.BlockSpec((1, 1, length), lambda e, j: (e, 0, 0)),
                column,
                up_spec,
                bias_spec,
                down_spec,
                last_spec,
            ],
            out_specs=out_specs,
            scratch_shapes=scratch,
        ),
        out_shape=out_shape,
        compiler_params=pltpu.CompilerParams(vmem_limit_bytes=60 << 20),
        cost_estimate=pl.CostEstimate(
            flops=(45 if train else 32) * 10**9,
            bytes_accessed=40 * 10**6,
            transcendentals=4 * 10**6,
        ),
        name="experts_new" if train else "experts_old",
    )(normed, cot, share, pos_row, pos_col, up_w[0], up_b, down_w[0], down_b)


def normalize(inputs):
    center = inputs - jnp.mean(inputs, axis=-1, keepdims=True)
    spread = jnp.mean(center * center, axis=-1, keepdims=True)
    scale = lax.rsqrt(spread + epsilon)
    return center * scale, scale


def normalize_back(unit, scale, grad):
    average = jnp.mean(grad, axis=-1, keepdims=True)
    along = jnp.mean(grad * unit, axis=-1, keepdims=True)
    return scale * (grad - average - unit * along)


def pack_experts(up, down):
    number, rows, width = up.shape[0], up.shape[1], down.shape[2]
    pieces = []
    for expert in range(number):
        for start in range(0, up.shape[2], width):
            pieces.append(up[expert, :, start : start + width])
        pieces.append(down[expert])
    return pieces


def expert_blocks(gathered, number, part, chunks):
    count, width = gathered.shape[0], gathered.shape[2]
    if part % 8 == 0:
        up = (gathered, part, lambda e, j: (0, 2 * chunks * e + j, 0))
        down = (gathered, chunks * part, lambda e, j: (j, 2 * e + 1, 0))
        return up, down
    both = gathered[:, : number * 2 * chunks * part].reshape(count, number, 2, -1, width)
    tall = both[:, :, 0].reshape(count, number, chunks, part, width).transpose(1, 2, 0, 3, 4)
    tall = tall.reshape(1, number * chunks * width, width)
    flat = both[:, :, 1].transpose(1, 0, 2, 3).reshape(1, number * chunks * width, width)
    place = lambda e, j: (0, chunks * e + j, 0)
    return (tall, width, place), (flat, width, place)


def by_owner(packed, number, part, chunks):
    width = packed.shape[2]
    count = width // part
    if part % 8 == 0:
        return packed
    both = packed.reshape(number, 2, chunks, width, width)
    up = both[:, 0].reshape(number, chunks, count, part, width).transpose(2, 0, 1, 3, 4)
    down = both[:, 1].reshape(number, count, chunks, part, width).transpose(1, 0, 2, 3, 4)
    return jnp.stack([up, down], axis=2).reshape(count, -1, width)


def scatter_sum(parts, order):
    wide = lax.axis_size("wide")
    bits = wide.bit_length() - 1
    names = list(range(bits - 1, -1, -1)) + ["narrow"]
    parts = parts.reshape((2,) * len(names) + parts.shape[1:])
    for name in order:
        at = names.index(name)
        names.pop(at)
        if name == "narrow":
            mine = lax.axis_index("narrow")
            swap = [(0, 1), (1, 0)]
            axis = "narrow"
        else:
            mine = (lax.axis_index("wide") >> name) & 1
            swap = [(index, index ^ (1 << name)) for index in range(wide)]
            axis = "wide"
        sent = lax.dynamic_index_in_dim(parts, 1 - mine, at, keepdims=False)
        kept = lax.dynamic_index_in_dim(parts, mine, at, keepdims=False)
        got = lax.ppermute(sent, axis, swap)
        parts = (kept.astype(f32) + got.astype(f32)).astype(bf16)
    return parts


def local(
    tokens,
    cotangent,
    segment_ids,
    routes,
    replay,
    gain_one,
    shift_one,
    w_query,
    b_query,
    w_key,
    w_value,
    b_value,
    w_out,
    b_out,
    gain_two,
    shift_two,
    w_router,
    new_up,
    new_up_bias,
    new_down,
    new_down_bias,
    old_up,
    old_up_bias,
    old_down,
    old_down_bias,
):
    seqs_here, length, width = tokens.shape
    part = w_query.shape[0]
    count = width // part
    hidden = new_up.shape[-1]
    new_count = new_up.shape[0]

    small = [gain_one, shift_one, b_query, b_value, b_out, gain_two, shift_two]
    small += [w_router, new_up_bias, old_up_bias, new_down_bias, old_down_bias]
    vector = jnp.concatenate([item.reshape(-1) for item in small])
    sizes = [item.size for item in small]
    vector = jnp.pad(vector, (0, 8 * width - vector.size)).reshape(8, width)
    chunks = hidden // width
    lead = pack_experts(new_up, new_down) + [w_query, w_key, w_value, w_out, vector]
    first = lax.all_gather(jnp.concatenate(lead, axis=0), AXES, axis=0)
    old_pack = jnp.concatenate(pack_experts(old_up, old_down), axis=0)
    old_all = lax.all_gather(old_pack, AXES, axis=0)

    base = new_count * 2 * chunks * part

    def weight_of(index):
        start = base + index * part
        return first[:, start : start + part].reshape(width, width)

    full_query, full_key, full_value, full_out = [weight_of(index) for index in range(4)]
    flat_small = first[:, base + 4 * part]
    marks = [0]
    for size in sizes:
        marks.append(marks[-1] + size)

    def vector_of(index):
        return flat_small[:, marks[index] : marks[index + 1]]

    seven = flat_small[:, : 7 * part].reshape(count, 7, part).transpose(1, 0, 2)
    seven = seven.reshape(7, width).astype(f32)
    gain_first, shift_first, bias_q, bias_v, bias_o, gain_second, shift_second = seven
    router = vector_of(7).reshape(width, EXPERTS)
    biases = []
    for index in (8, 9, 10, 11):
        item = vector_of(index).reshape(count, new_count, -1).transpose(1, 0, 2)
        biases.append(item.reshape(new_count, 1, -1))
    new_up_b, old_up_b, new_down_b, old_down_b = biases

    flat = tokens.reshape(length, width).astype(f32)
    cot = cotangent.reshape(length, width)
    segments = segment_ids.reshape(length)
    route_flat = routes.reshape(length, -1)
    member = jnp.any(
        route_flat[:, :, None] == jnp.arange(EXPERTS, dtype=jnp.int32)[None, None, :], axis=1
    )
    member_int = member.astype(jnp.int32)
    running = jnp.cumsum(member_int, axis=0)
    position = jnp.where(member, running - 1, -1)
    pos_row = position.T[:, None, :]
    pos_col = position.T[:, :, None]

    unit_one, scale_one = normalize(flat)
    normed = (unit_one * gain_first + shift_first).astype(bf16)
    query = (dot(normed, full_query) + bias_q).astype(bf16)
    keys = dot(normed, full_key).astype(bf16)
    values = (dot(normed, full_value) + bias_v).astype(bf16)
    mixed, probs = attn_forward(query, keys, values, segments[:, None], segments[None, :])
    resid = flat + dot(mixed, full_out) + bias_o
    unit_two, scale_two = normalize(resid)
    normed_two = (unit_two * gain_second + shift_second).astype(bf16)
    logits = dot(normed_two, router)
    trained = (jnp.arange(EXPERTS) >= FROZEN).astype(f32)
    keep = 1.0 - replay.reshape(length, 1).astype(f32) * trained

    def gate_map(values_in):
        gate = jax.nn.softmax(values_in, axis=-1)
        picked = jnp.where(member, gate, 0.0)
        return picked / jnp.sum(picked, axis=-1, keepdims=True) * keep

    share, gate_back = jax.vjp(gate_map, logits)
    share_cols = share.T[:, :, None]

    got = experts(
        True,
        normed_two,
        cot,
        share_cols[FROZEN:],
        pos_row[FROZEN:],
        pos_col[FROZEN:],
        *expert_blocks(first, new_count, part, chunks),
        new_up_b,
        new_down_b,
    )
    out_new, gx_new, gc_new, grad_up_b, grad_down_b, packed = got
    packed = by_owner(packed, new_count, part, chunks).reshape(-1, width)
    summed_new = lax.psum_scatter(packed, AXES, scatter_dimension=0, tiled=True)
    summed_new = summed_new.reshape(new_count, 2, chunks * part, width).astype(f32)
    sum_up = summed_new[:, 0].reshape(new_count, chunks, part, width).transpose(0, 2, 1, 3)
    sum_up = sum_up.reshape(new_count, part, hidden)
    sum_down = summed_new[:, 1]

    out_old, gx_old, gc_old = experts(
        False,
        normed_two,
        cot,
        share_cols[:FROZEN],
        pos_row[:FROZEN],
        pos_col[:FROZEN],
        *expert_blocks(old_all, old_up.shape[0], part, chunks),
        old_up_b,
        old_down_b,
    )
    result = (resid + out_new + out_old).astype(bf16)
    grad_share = jnp.concatenate([gc_old, gc_new], axis=0)[:, :, 0].T
    grad_logits = gate_back(grad_share)[0]
    grad_router = lax.dot_general(
        normed_two.astype(f32),
        grad_logits,
        (((0,), (0,)), ((), ())),
        precision=lax.Precision.HIGHEST,
        preferred_element_type=f32,
    )
    grad_two = gx_new + gx_old
    for expert in range(EXPERTS):
        grad_two = grad_two + grad_logits[:, expert : expert + 1] * router[:, expert].astype(f32)
    grad_two = grad_two.astype(bf16).astype(f32)
    grad_gain_two = jnp.sum(grad_two * unit_two, axis=0)
    grad_shift_two = jnp.sum(grad_two, axis=0)
    grad_resid = cot.astype(f32) + normalize_back(unit_two, scale_two, grad_two * gain_second)
    grad_attn = grad_resid.astype(bf16)
    grad_w_out = dot_tn(mixed, grad_attn)
    grad_b_out = jnp.sum(grad_attn.astype(f32), axis=0)
    grad_mixed = dot_nt(grad_attn, full_out).astype(bf16)
    grad_q, grad_k, grad_v = attn_backward(query, keys, values, grad_mixed, probs)
    grad_w_query = dot_tn(normed, grad_q)
    grad_w_key = dot_tn(normed, grad_k)
    grad_w_value = dot_tn(normed, grad_v)
    grad_b_query = jnp.sum(grad_q.astype(f32), axis=0)
    grad_b_value = jnp.sum(grad_v.astype(f32), axis=0)
    grad_one = dot_nt(grad_q, full_query) + dot_nt(grad_k, full_key) + dot_nt(grad_v, full_value)
    grad_one = grad_one.astype(bf16).astype(f32)
    grad_gain_one = jnp.sum(grad_one * unit_one, axis=0)
    grad_shift_one = jnp.sum(grad_one, axis=0)
    grad_input = grad_resid + normalize_back(unit_one, scale_one, grad_one * gain_first)

    bits = list(range(2, lax.axis_size("wide").bit_length() - 1))
    one_way = [0, 1, "narrow"] + bits
    other_way = [0, "narrow", 1] + bits
    sum_out = scatter_sum(grad_w_out.reshape(count, part, width).astype(bf16), one_way)
    pieces = [
        item.reshape(count, part, width).astype(bf16)
        for item in (grad_w_query, grad_w_key, grad_w_value)
    ]
    vectors = [grad_gain_one, grad_shift_one, grad_b_query, grad_b_value, grad_b_out]
    vectors += [grad_gain_two, grad_shift_two, grad_router]
    rows = [item.reshape(count, -1) for item in vectors]
    for item in (grad_up_b, grad_down_b):
        rows.append(item.reshape(new_count, count, -1).transpose(1, 0, 2).reshape(count, -1))
    lengths = [item.shape[1] for item in rows]
    row = jnp.concatenate(rows, axis=1).astype(bf16)
    row = jnp.pad(row, ((0, 0), (0, 8 * width - row.shape[1]))).reshape(count, 8, width)
    last = jnp.concatenate(pieces + [row], axis=1)
    middle = last.shape[1] // 2
    halves = [scatter_sum(last[:, :middle], one_way), scatter_sum(last[:, middle:], other_way)]
    summed = jnp.concatenate(halves, axis=0).astype(f32)
    sums = [summed[index * part : (index + 1) * part] for index in range(3)]
    sums.append(sum_out.astype(f32))
    tail = summed[3 * part]
    found = []
    at = 0
    for size in lengths:
        found.append(tail[at : at + size])
        at += size
    return (
        result.reshape(seqs_here, length, width),
        grad_input.astype(bf16).reshape(seqs_here, length, width),
        found[0],
        found[1],
        sums[0],
        found[2],
        sums[1],
        sums[2],
        found[3],
        sums[3],
        found[4],
        found[5],
        found[6],
        found[7].reshape(part, EXPERTS),
        sum_up,
        found[8].reshape(new_count, -1),
        sum_down,
        found[9].reshape(new_count, -1),
    )


def solution(mesh):
    axes = AXES
    rows3 = P(axes, None, None)
    rows2 = P(axes, None)
    rows1 = P(axes)
    mid3 = P(None, axes, None)
    mid2 = P(None, axes)
    placed = (rows3, rows3, rows2, rows3, rows2)
    placed += (rows1, rows1, rows2, rows1, rows2, rows2, rows1, rows2, rows1, rows1, rows1, rows2)
    placed += (mid3, mid2) * 4
    outs = (rows3, rows3, rows1, rows1, rows2, rows1, rows2, rows2, rows1, rows2, rows1)
    outs += (rows1, rows1, rows2, mid3, mid2, mid3, mid2)
    return jax.shard_map(local, mesh=mesh, in_specs=placed, out_specs=outs, check_vma=False)
```

```python
import functools

import jax
import jax.numpy as jnp
from jax import lax
from jax.experimental import pallas as pl
from jax.experimental.pallas import tpu as pltpu
from jax.sharding import PartitionSpec as P

HD = 64
FROZEN = 2
EXPERTS = 4
CAP = 640
BLOCK = 256
LONGEST = 512
AXES = ("wide", "narrow")

epsilon = 1e-05
masked_score = -1e30
f32 = jnp.float32
bf16 = jnp.bfloat16


def dot(a, b):
    return jnp.dot(a, b, preferred_element_type=f32)


def dot_nt(a, b):
    return lax.dot_general(a, b, (((1,), (1,)), ((), ())), preferred_element_type=f32)


def dot_tn(a, b):
    return lax.dot_general(a, b, (((0,), (0,)), ((), ())), preferred_element_type=f32)


def band(index):
    start = max(0, index - LONGEST // BLOCK) * BLOCK
    return start, (index + 1) * BLOCK - start


def attn_forward_kernel(q_ref, k_ref, v_ref, seg_col, seg_row, out_ref, prob_ref):
    length = q_ref.shape[0]
    first = lax.broadcasted_iota(jnp.int32, (BLOCK, 2 * HD), 1) < HD
    for index in range(length // BLOCK):
        start, size = band(index)
        rows = pl.ds(index * BLOCK, BLOCK)
        cols = pl.ds(start, size)
        place_q = lax.broadcasted_iota(jnp.int32, (BLOCK, size), 0) + (index * BLOCK - start)
        place_k = lax.broadcasted_iota(jnp.int32, (BLOCK, size), 1)
        allowed = (seg_col[rows, :] == seg_row[:, cols]) & (place_q >= place_k)
        query = q_ref[rows, :] * jnp.asarray(HD**-0.5, bf16)
        zero = jnp.zeros_like(query)
        keys = k_ref[cols, :]
        values = v_ref[cols, :]
        parts = []
        for head in range(2):
            mine = first if head == 0 else jnp.logical_not(first)
            scores = dot_nt(jnp.where(mine, query, zero), keys)
            scores = jnp.where(allowed, scores, masked_score)
            expon = jnp.exp(scores - jnp.max(scores, axis=-1, keepdims=True))
            total = jnp.sum(expon, axis=-1, keepdims=True)
            weights = (expon * (1.0 / total)).astype(bf16)
            prob_ref[head, rows, pl.ds(0, size)] = weights
            parts.append(dot(weights, values))
        out_ref[rows, :] = jnp.where(first, parts[0], parts[1]).astype(bf16)


def attn_forward(query, keys, values, seg_col, seg_row):
    length, width = query.shape
    pairs = width // (2 * HD)
    span = min(length, LONGEST + BLOCK)
    col = pl.BlockSpec((length, 2 * HD), lambda p: (0, p))
    return pl.pallas_call(
        attn_forward_kernel,
        grid=(pairs,),
        in_specs=[
            col,
            col,
            col,
            pl.BlockSpec((length, 1), lambda p: (0, 0)),
            pl.BlockSpec((1, length), lambda p: (0, 0)),
        ],
        out_specs=[col, pl.BlockSpec((2, length, span), lambda p: (p, 0, 0))],
        out_shape=[
            jax.ShapeDtypeStruct((length, width), bf16),
            jax.ShapeDtypeStruct((2 * pairs, length, span), bf16),
        ],
        compiler_params=pltpu.CompilerParams(vmem_limit_bytes=60 << 20),
        cost_estimate=pl.CostEstimate(
            flops=20 * 10**9, bytes_accessed=30 * 10**6, transcendentals=8 * 10**6
        ),
        name="attn_forward",
    )(query, keys, values, seg_col, seg_row)


def attn_backward_kernel(q_ref, k_ref, v_ref, grad_ref, prob_ref, gq_ref, gk_ref, gv_ref, gk, gv):
    length = q_ref.shape[0]
    first = lax.broadcasted_iota(jnp.int32, (BLOCK, 2 * HD), 1) < HD
    gk[...] = jnp.zeros_like(gk)
    gv[...] = jnp.zeros_like(gv)
    for index in range(length // BLOCK):
        start, size = band(index)
        rows = pl.ds(index * BLOCK, BLOCK)
        cols = pl.ds(start, size)
        query = q_ref[rows, :]
        grad = grad_ref[rows, :]
        keys = k_ref[cols, :]
        values = v_ref[cols, :]
        zero = jnp.zeros_like(query)
        parts = []
        for head in range(2):
            mine = first if head == 0 else jnp.logical_not(first)
            grad_head = jnp.where(mine, grad, zero)
            probs = prob_ref[head, rows, pl.ds(0, size)]
            grad_weights = dot_nt(grad_head, values)
            wide = probs.astype(f32)
            inner = jnp.sum(wide * grad_weights, axis=-1, keepdims=True)
            grad_scores = (wide * (grad_weights - inner)).astype(bf16)
            parts.append(dot(grad_scores, keys))
            gk[cols, :] += dot_tn(grad_scores, jnp.where(mine, query, zero))
            gv[cols, :] += dot_tn(probs, grad_head)
        gq_ref[rows, :] = (jnp.where(first, parts[0], parts[1]) * HD**-0.5).astype(bf16)
    gk_ref[...] = (gk[...] * HD**-0.5).astype(bf16)
    gv_ref[...] = gv[...].astype(bf16)


def attn_backward(query, keys, values, grad, probs):
    length, width = query.shape
    pairs = width // (2 * HD)
    span = probs.shape[-1]
    col = pl.BlockSpec((length, 2 * HD), lambda p: (0, p))
    shape = jax.ShapeDtypeStruct((length, width), bf16)
    return pl.pallas_call(
        attn_backward_kernel,
        grid=(pairs,),
        in_specs=[col, col, col, col, pl.BlockSpec((2, length, span), lambda p: (p, 0, 0))],
        out_specs=[col, col, col],
        out_shape=[shape, shape, shape],
        scratch_shapes=[pltpu.VMEM((length, 2 * HD), f32), pltpu.VMEM((length, 2 * HD), f32)],
        compiler_params=pltpu.CompilerParams(vmem_limit_bytes=60 << 20),
        cost_estimate=pl.CostEstimate(
            flops=50 * 10**9, bytes_accessed=30 * 10**6, transcendentals=0
        ),
        name="attn_backward",
    )(query, keys, values, grad, probs)


def expert_kernel(train, chunks, *refs):
    inputs, outputs = refs[:9], refs[9 : 9 + (6 if train else 3)]
    scratch = refs[9 + len(outputs) :]
    normed, cot, share, pos_row, pos_col, up_block, up_b, down_block, down_b = inputs
    out_ref, gx_ref, gc_ref = outputs[:3]
    rows_x, rows_g, rows_out, rows_gx = scratch[:4]
    expert, chunk = pl.program_id(0), pl.program_id(1)
    last = chunks - 1
    length, width = normed.shape
    wide = up_block.shape[-1]
    up_w = up_block.reshape(width, wide)
    down_w = down_block.reshape(wide, width)

    if train:
        pack_ref = outputs[5]
        up_out, down_out, sems = scratch[4:]
        part = up_out.shape[1]
        group, tall = down_out.shape[:2]
        split = tall == (last + 1) * part

        def copies(which_expert, which_chunk):
            base = which_expert * (2 * (last + 1) * part)
            up_at = pl.multiple_of(base + which_chunk * part, 8)
            down_at = base + (last + 1) * part + (0 if split else which_chunk * tall)
            down_at = pl.multiple_of(down_at, 8)
            first = which_chunk * group if split else 0
            return (
                pltpu.make_async_copy(up_out, pack_ref.at[:, pl.ds(up_at, part), :], sems.at[0]),
                pltpu.make_async_copy(
                    down_out, pack_ref.at[pl.ds(first, group), pl.ds(down_at, tall), :], sems.at[1]
                ),
            )

    @pl.when((expert == 0) & (chunk == 0))
    def _():
        out_ref[...] = jnp.zeros_like(out_ref)
        gx_ref[...] = jnp.zeros_like(gx_ref)

    @pl.when(chunk == 0)
    def _():
        slots = lax.broadcasted_iota(jnp.int32, (CAP, length), 0)
        select = (slots == pos_row[0]).astype(bf16)
        rows_x[...] = dot(select, normed[...]).astype(bf16)
        scaled = (cot[...].astype(f32) * share[0]).astype(bf16)
        grads = dot(select, scaled)
        rows_g[...] = grads.astype(bf16)
        rows_out[...] = jnp.broadcast_to(down_b[0].astype(f32), rows_out.shape)
        rows_gx[...] = jnp.zeros_like(rows_gx)
        if train:
            outputs[4][0] = jnp.sum(grads, axis=0, keepdims=True)

    bias = up_b[0].astype(f32)

    up = dot(rows_x[...], up_w[...]) + bias
    back = dot_nt(rows_g[...], down_w[...])
    square = up * up
    bent = jnp.tanh(up * (0.7978845608028654 + (0.7978845608028654 * 0.044715) * square))
    half = 0.5 + 0.5 * bent
    active = (up * half).astype(bf16)
    slope = half + up * (half - half * bent) * (
        0.7978845608028654 + (3 * 0.044715 * 0.7978845608028654) * square
    )
    grad_up = (back * slope).astype(bf16)
    rows_out[...] += dot(active, down_w[...])
    rows_gx[...] += dot_nt(grad_up, up_w[...])
    if train:
        outputs[3][0] = jnp.sum(grad_up.astype(f32), axis=0, keepdims=True)
        previous = jnp.maximum(expert * (last + 1) + chunk - 1, 0)

        @pl.when((expert > 0) | (chunk > 0))
        def _():
            for copy in copies(previous // (last + 1), lax.rem(previous, last + 1)):
                copy.wait()

        up_out.reshape(width, wide)[...] = dot_tn(rows_x[...], grad_up).astype(bf16)
        down_out.reshape(wide, width)[...] = dot_tn(active, rows_g[...]).astype(bf16)
        for copy in copies(expert, chunk):
            copy.start()

        @pl.when((expert == pl.num_programs(0) - 1) & (chunk == last))
        def _():
            for copy in copies(expert, chunk):
                copy.wait()

    @pl.when(chunk == last)
    def _():
        slots = lax.broadcasted_iota(jnp.int32, (length, CAP), 1)
        select = (slots == pos_col[0]).astype(bf16)
        expert_out = dot(select, rows_out[...].astype(bf16))
        gc_ref[0] = jnp.sum(cot[...].astype(f32) * expert_out, axis=-1, keepdims=True)
        out_ref[...] += share[0] * expert_out
        gx_ref[...] += dot(select, rows_gx[...].astype(bf16))


def experts(train, normed, cot, share, pos_row, pos_col, up_w, down_w, up_b, down_b):
    length, width = normed.shape
    number, hidden = up_b.shape[0], up_b.shape[2]
    chunks = hidden // width
    whole = pl.BlockSpec((length, width), lambda e, j: (0, 0))
    column = pl.BlockSpec((1, length, 1), lambda e, j: (e, 0, 0))
    up_spec = pl.BlockSpec((width // up_w[1], up_w[1], width), up_w[2])
    down_spec = pl.BlockSpec((width // down_w[1], down_w[1], width), down_w[2])
    bias_spec = pl.BlockSpec((1, 1, width), lambda e, j: (e, 0, j))
    last_spec = pl.BlockSpec((1, 1, width), lambda e, j: (e, 0, 0))
    out_specs = [whole, whole, column]
    out_shape = [
        jax.ShapeDtypeStruct((length, width), f32),
        jax.ShapeDtypeStruct((length, width), f32),
        jax.ShapeDtypeStruct((number, length, 1), f32),
    ]
    scratch = [
        pltpu.VMEM((CAP, width), bf16),
        pltpu.VMEM((CAP, width), bf16),
        pltpu.VMEM((CAP, width), f32),
        pltpu.VMEM((CAP, width), f32),
    ]
    if train:
        part, tall = up_w[1], down_w[1]
        out_specs += [bias_spec, last_spec, pl.BlockSpec(memory_space=pl.ANY)]
        out_shape += [
            jax.ShapeDtypeStruct(up_b.shape, f32),
            jax.ShapeDtypeStruct(down_b.shape, f32),
            jax.ShapeDtypeStruct((width // part, number * 2 * chunks * part, width), bf16),
        ]
        scratch += [
            pltpu.VMEM((width // part, part, width), bf16),
            pltpu.VMEM((width // tall, tall, width), bf16),
            pltpu.SemaphoreType.DMA((2,)),
        ]
    return pl.pallas_call(
        functools.partial(expert_kernel, train, chunks),
        grid_spec=pltpu.PrefetchScalarGridSpec(
            num_scalar_prefetch=0,
            grid=(number, chunks),
            in_specs=[
                whole,
                whole,
                column,
                pl.BlockSpec((1, 1, length), lambda e, j: (e, 0, 0)),
                column,
                up_spec,
                bias_spec,
                down_spec,
                last_spec,
            ],
            out_specs=out_specs,
            scratch_shapes=scratch,
        ),
        out_shape=out_shape,
        compiler_params=pltpu.CompilerParams(vmem_limit_bytes=60 << 20),
        cost_estimate=pl.CostEstimate(
            flops=(45 if train else 32) * 10**9,
            bytes_accessed=40 * 10**6,
            transcendentals=4 * 10**6,
        ),
        name="experts_new" if train else "experts_old",
    )(normed, cot, share, pos_row, pos_col, up_w[0], up_b, down_w[0], down_b)


def normalize(inputs):
    center = inputs - jnp.mean(inputs, axis=-1, keepdims=True)
    spread = jnp.mean(center * center, axis=-1, keepdims=True)
    scale = lax.rsqrt(spread + epsilon)
    return center * scale, scale


def normalize_back(unit, scale, grad):
    average = jnp.mean(grad, axis=-1, keepdims=True)
    along = jnp.mean(grad * unit, axis=-1, keepdims=True)
    return scale * (grad - average - unit * along)


def pack_experts(up, down):
    pieces = []
    width = down.shape[2]
    for expert in range(up.shape[0]):
        for start in range(0, up.shape[2], width):
            pieces.append(up[expert, :, start : start + width])
        pieces.append(down[expert])
    return pieces


def pack_small(shape, seven, router, new_ub, old_ub, new_db, old_db):
    places = ((seven, 0, 0), (router, 0, 128), (new_db, 4, 128), (old_db, 6, 128))
    places += ((new_ub, 0, 256), (old_ub, 2, 256))
    total = jnp.zeros(shape, bf16)
    for item, row, col in places:
        edges = ((row, shape[0] - row - item.shape[0]), (col, shape[1] - col - item.shape[1]))
        total = total + jnp.pad(item, edges)
    return total


def pack_kernel(new_up, new_down, old_up, old_down, w_q, w_k, w_v, small, new_out, old_out, a, b):
    for up, down, out in ((new_up, new_down, new_out), (old_up, old_down, old_out)):
        number, part, hidden = up.shape
        width = down.shape[2]
        at = 0
        for expert in range(number):
            for start in range(0, hidden, width):
                out[at : at + part, :] = up[expert, :, start : start + width]
                at += part
            out[at : at + down.shape[1], :] = down[expert]
            at += down.shape[1]
    part = w_q.shape[0]
    cut = a.shape[0] - part
    a[:part, :] = w_q[...]
    a[part:, :] = w_k[:cut, :]
    b[: part - cut, :] = w_k[cut:, :]
    b[part - cut : 2 * part - cut, :] = w_v[...]
    b[2 * part - cut :, :] = small[...]


def pack_all(new_up, new_down, old_up, old_down, w_query, w_key, w_value, small):
    part, width = w_query.shape
    if part % 8:
        new_pack = jnp.concatenate(pack_experts(new_up, new_down), axis=0)
        old_pack = jnp.concatenate(pack_experts(old_up, old_down), axis=0)
        head = jnp.concatenate([w_query, w_key, w_value, small], axis=0)
        middle = part + part // 2
        return new_pack, old_pack, head[:middle], head[middle:]
    rows = new_up.size // width + new_down.size // width
    half = (3 * part + 8) // 16 * 8
    shapes = [(rows, width), (rows, width), (half, width), (3 * part + 8 - half, width)]
    return pl.pallas_call(
        pack_kernel,
        out_shape=[jax.ShapeDtypeStruct(shape, bf16) for shape in shapes],
        name="pack",
    )(new_up, new_down, old_up, old_down, w_query, w_key, w_value, small)


def swap_of(name):
    if name == "narrow":
        return "narrow", lax.axis_index("narrow"), [(0, 1), (1, 0)]
    wide = lax.axis_size("wide")
    pairs = [(index, index ^ (1 << name)) for index in range(wide)]
    return "wide", (lax.axis_index("wide") >> name) & 1, pairs


def gather_all(mine, order):
    names = []
    held = mine
    for name in order:
        axis, bit, pairs = swap_of(name)
        got = lax.ppermute(held, axis, pairs)
        rank = -1 if name == "narrow" else name
        at = sum(1 for item in names if item > rank)
        names.insert(at, rank)
        low = jnp.stack([held, got], axis=at)
        high = jnp.stack([got, held], axis=at)
        held = jnp.where(bit == 0, low, high)
    return held.reshape((-1,) + mine.shape)


def expert_blocks(gathered, number, part, chunks):
    count, width = gathered.shape[0], gathered.shape[2]
    if part % 8 == 0:
        up = (gathered, part, lambda e, j: (0, 2 * chunks * e + j, 0))
        down = (gathered, chunks * part, lambda e, j: (j, 2 * e + 1, 0))
        return up, down
    both = gathered[:, : number * 2 * chunks * part].reshape(count, number, 2, -1, width)
    tall = both[:, :, 0].reshape(count, number, chunks, part, width).transpose(1, 2, 0, 3, 4)
    tall = tall.reshape(1, number * chunks * width, width)
    flat = both[:, :, 1].transpose(1, 0, 2, 3).reshape(1, number * chunks * width, width)
    place = lambda e, j: (0, chunks * e + j, 0)
    return (tall, width, place), (flat, width, place)


def by_owner(packed, number, part, chunks):
    width = packed.shape[2]
    count = width // part
    if part % 8 == 0:
        return packed
    both = packed.reshape(number, 2, chunks, width, width)
    up = both[:, 0].reshape(number, chunks, count, part, width).transpose(2, 0, 1, 3, 4)
    down = both[:, 1].reshape(number, count, chunks, part, width).transpose(1, 0, 2, 3, 4)
    return jnp.stack([up, down], axis=2).reshape(count, -1, width)


def scatter_sum(parts, order):
    bits = lax.axis_size("wide").bit_length() - 1
    names = list(range(bits - 1, -1, -1)) + ["narrow"]
    parts = parts.reshape((2,) * len(names) + parts.shape[1:])
    for name in order:
        at = names.index(name)
        names.pop(at)
        axis, mine, swap = swap_of(name)
        sent = lax.dynamic_index_in_dim(parts, 1 - mine, at, keepdims=False)
        kept = lax.dynamic_index_in_dim(parts, mine, at, keepdims=False)
        got = lax.ppermute(sent, axis, swap)
        parts = (kept.astype(f32) + got.astype(f32)).astype(bf16)
    return parts


def local(
    tokens,
    cotangent,
    segment_ids,
    routes,
    replay,
    gain_one,
    shift_one,
    w_query,
    b_query,
    w_key,
    w_value,
    b_value,
    w_out,
    b_out,
    gain_two,
    shift_two,
    w_router,
    new_up,
    new_up_bias,
    new_down,
    new_down_bias,
    old_up,
    old_up_bias,
    old_down,
    old_down_bias,
):
    seqs_here, length, width = tokens.shape
    part = w_query.shape[0]
    count = width // part
    hidden = new_up.shape[-1]
    new_count = new_up.shape[0]

    chunks = hidden // width
    bits = list(range(2, lax.axis_size("wide").bit_length() - 1))
    one_way = [0, 1, "narrow"] + bits
    other_way = [0, "narrow", 1] + bits

    seven = jnp.stack([gain_one, shift_one, b_query, b_value, b_out, gain_two, shift_two])
    small = pack_small(
        (8, width),
        seven,
        w_router.T,
        new_up_bias,
        old_up_bias,
        new_down_bias,
        old_down_bias,
    )
    new_pack, old_pack, head_a, head_b = pack_all(
        new_up, new_down, old_up, old_down, w_query, w_key, w_value, small
    )
    new_all = lax.all_gather(new_pack, AXES, axis=0)
    old_all = lax.all_gather(old_pack, AXES, axis=0)
    all_a = gather_all(head_a, one_way[::-1])
    all_b = gather_all(head_b, other_way[::-1])
    full_out = gather_all(w_out, one_way[::-1]).reshape(width, width)
    cut = head_a.shape[0] - part
    full_query = all_a[:, :part].reshape(width, width)
    full_key = jnp.concatenate([all_a[:, part:], all_b[:, : part - cut]], axis=1)
    full_key = full_key.reshape(width, width)
    full_value = all_b[:, part - cut : 2 * part - cut].reshape(width, width)
    block = all_b[:, 2 * part - cut :]

    def columns(row, rows, col, wide):
        return block[:, row : row + rows, col : col + wide].transpose(1, 0, 2).reshape(rows, -1)

    seven = columns(0, 7, 0, part).astype(f32)
    gain_first, shift_first, bias_q, bias_v, bias_o, gain_second, shift_second = seven
    router = columns(0, EXPERTS, 128, part).T
    new_down_b = columns(4, new_count, 128, part)[:, None, :]
    old_down_b = columns(6, new_count, 128, part)[:, None, :]
    new_up_b = columns(0, new_count, 256, new_up_bias.shape[1])[:, None, :]
    old_up_b = columns(2, new_count, 256, new_up_bias.shape[1])[:, None, :]

    flat = tokens.reshape(length, width).astype(f32)
    cot = cotangent.reshape(length, width)
    segments = segment_ids.reshape(length)
    route_flat = routes.reshape(length, -1)
    member = jnp.any(
        route_flat[:, :, None] == jnp.arange(EXPERTS, dtype=jnp.int32)[None, None, :], axis=1
    )
    member_int = member.astype(jnp.int32)
    running = jnp.cumsum(member_int, axis=0)
    position = jnp.where(member, running - 1, -1)
    pos_row = position.T[:, None, :]
    pos_col = position.T[:, :, None]

    unit_one, scale_one = normalize(flat)
    normed = (unit_one * gain_first + shift_first).astype(bf16)
    query = (dot(normed, full_query) + bias_q).astype(bf16)
    keys = dot(normed, full_key).astype(bf16)
    values = (dot(normed, full_value) + bias_v).astype(bf16)
    mixed, probs = attn_forward(query, keys, values, segments[:, None], segments[None, :])
    resid = flat + dot(mixed, full_out) + bias_o
    unit_two, scale_two = normalize(resid)
    normed_two = (unit_two * gain_second + shift_second).astype(bf16)
    logits = dot(normed_two, router)
    trained = (jnp.arange(EXPERTS) >= FROZEN).astype(f32)
    keep = 1.0 - replay.reshape(length, 1).astype(f32) * trained

    def gate_map(values_in):
        gate = jax.nn.softmax(values_in, axis=-1)
        picked = jnp.where(member, gate, 0.0)
        return picked / jnp.sum(picked, axis=-1, keepdims=True) * keep

    share, gate_back = jax.vjp(gate_map, logits)
    share_cols = share.T[:, :, None]

    got = experts(
        True,
        normed_two,
        cot,
        share_cols[FROZEN:],
        pos_row[FROZEN:],
        pos_col[FROZEN:],
        *expert_blocks(new_all, new_count, part, chunks),
        new_up_b,
        new_down_b,
    )
    out_new, gx_new, gc_new, grad_up_b, grad_down_b, packed = got
    packed = by_owner(packed, new_count, part, chunks).reshape(-1, width)
    summed_new = lax.psum_scatter(packed, AXES, scatter_dimension=0, tiled=True)
    summed_new = summed_new.reshape(new_count, 2, chunks * part, width).astype(f32)
    sum_up = summed_new[:, 0].reshape(new_count, chunks, part, width).transpose(0, 2, 1, 3)
    sum_up = sum_up.reshape(new_count, part, hidden)
    sum_down = summed_new[:, 1]

    out_old, gx_old, gc_old = experts(
        False,
        normed_two,
        cot,
        share_cols[:FROZEN],
        pos_row[:FROZEN],
        pos_col[:FROZEN],
        *expert_blocks(old_all, old_up.shape[0], part, chunks),
        old_up_b,
        old_down_b,
    )
    result = (resid + out_new + out_old).astype(bf16)
    grad_share = jnp.concatenate([gc_old, gc_new], axis=0)[:, :, 0].T
    grad_logits = gate_back(grad_share)[0]
    grad_router = lax.dot_general(
        normed_two.astype(f32),
        grad_logits,
        (((0,), (0,)), ((), ())),
        precision=lax.Precision.HIGHEST,
        preferred_element_type=f32,
    )
    grad_two = gx_new + gx_old
    for expert in range(EXPERTS):
        grad_two = grad_two + grad_logits[:, expert : expert + 1] * router[:, expert].astype(f32)
    grad_two = grad_two.astype(bf16).astype(f32)
    grad_gain_two = jnp.sum(grad_two * unit_two, axis=0)
    grad_shift_two = jnp.sum(grad_two, axis=0)
    grad_resid = cot.astype(f32) + normalize_back(unit_two, scale_two, grad_two * gain_second)
    grad_attn = grad_resid.astype(bf16)
    grad_w_out = dot_tn(mixed, grad_attn)
    grad_b_out = jnp.sum(grad_attn.astype(f32), axis=0)
    grad_w_out = grad_w_out.reshape(count, part, width).astype(bf16)
    grad_w_out, grad_attn = lax.optimization_barrier((grad_w_out, grad_attn))
    sum_out = scatter_sum(grad_w_out, one_way)
    grad_mixed = dot_nt(grad_attn, full_out).astype(bf16)
    grad_q, grad_k, grad_v = attn_backward(query, keys, values, grad_mixed, probs)
    grad_w_query = dot_tn(normed, grad_q)
    grad_w_key = dot_tn(normed, grad_k)
    grad_w_value = dot_tn(normed, grad_v)
    grad_b_query = jnp.sum(grad_q.astype(f32), axis=0)
    grad_b_value = jnp.sum(grad_v.astype(f32), axis=0)
    grad_one = dot_nt(grad_q, full_query) + dot_nt(grad_k, full_key) + dot_nt(grad_v, full_value)
    grad_one = grad_one.astype(bf16).astype(f32)
    grad_gain_one = jnp.sum(grad_one * unit_one, axis=0)
    grad_shift_one = jnp.sum(grad_one, axis=0)
    grad_input = grad_resid + normalize_back(unit_one, scale_one, grad_one * gain_first)

    pieces = [
        item.reshape(count, part, width).astype(bf16)
        for item in (grad_w_query, grad_w_key, grad_w_value)
    ]
    vectors = [grad_gain_one, grad_shift_one, grad_b_query, grad_b_value, grad_b_out]
    vectors += [grad_gain_two, grad_shift_two, grad_router]
    rows = [item.reshape(count, -1) for item in vectors]
    for item in (grad_up_b, grad_down_b):
        rows.append(item.reshape(new_count, count, -1).transpose(1, 0, 2).reshape(count, -1))
    lengths = [item.shape[1] for item in rows]
    row = jnp.concatenate(rows, axis=1).astype(bf16)
    row = jnp.pad(row, ((0, 0), (0, 8 * width - row.shape[1]))).reshape(count, 8, width)
    last = jnp.concatenate(pieces + [row], axis=1)
    middle = last.shape[1] // 2
    halves = [scatter_sum(last[:, :middle], one_way), scatter_sum(last[:, middle:], other_way)]
    summed = jnp.concatenate(halves, axis=0).astype(f32)
    sums = [summed[index * part : (index + 1) * part] for index in range(3)]
    sums.append(sum_out.astype(f32))
    tail = summed[3 * part]
    found = []
    at = 0
    for size in lengths:
        found.append(tail[at : at + size])
        at += size
    return (
        result.reshape(seqs_here, length, width),
        grad_input.astype(bf16).reshape(seqs_here, length, width),
        found[0],
        found[1],
        sums[0],
        found[2],
        sums[1],
        sums[2],
        found[3],
        sums[3],
        found[4],
        found[5],
        found[6],
        found[7].reshape(part, EXPERTS),
        sum_up,
        found[8].reshape(new_count, -1),
        sum_down,
        found[9].reshape(new_count, -1),
    )


def solution(mesh):
    axes = AXES
    rows3 = P(axes, None, None)
    rows2 = P(axes, None)
    rows1 = P(axes)
    mid3 = P(None, axes, None)
    mid2 = P(None, axes)
    placed = (rows3, rows3, rows2, rows3, rows2)
    placed += (rows1, rows1, rows2, rows1, rows2, rows2, rows1, rows2, rows1, rows1, rows1, rows2)
    placed += (mid3, mid2) * 4
    outs = (rows3, rows3, rows1, rows1, rows2, rows1, rows2, rows2, rows1, rows2, rows1)
    outs += (rows1, rows1, rows2, mid3, mid2, mid3, mid2)
    return jax.shard_map(local, mesh=mesh, in_specs=placed, out_specs=outs, check_vma=False)
```

```python
import functools

import jax
import jax.numpy as jnp
from jax import lax
from jax.experimental import pallas as pl
from jax.experimental.pallas import tpu as pltpu
from jax.sharding import PartitionSpec as P

HD = 64
FROZEN = 2
EXPERTS = 4
CAP = 640
BLOCK = 256
LONGEST = 512
AXES = ("wide", "narrow")

epsilon = 1e-05
masked_score = -1e30
f32 = jnp.float32
bf16 = jnp.bfloat16


def dot(a, b):
    return jnp.dot(a, b, preferred_element_type=f32)


def dot_nt(a, b):
    return lax.dot_general(a, b, (((1,), (1,)), ((), ())), preferred_element_type=f32)


def dot_tn(a, b):
    return lax.dot_general(a, b, (((0,), (0,)), ((), ())), preferred_element_type=f32)


def band(index):
    start = max(0, index - LONGEST // BLOCK) * BLOCK
    return start, (index + 1) * BLOCK - start


def attn_forward_kernel(q_ref, k_ref, v_ref, seg_col, seg_row, out_ref, prob_ref):
    length = q_ref.shape[0]
    first = lax.broadcasted_iota(jnp.int32, (BLOCK, 2 * HD), 1) < HD
    for index in range(length // BLOCK):
        start, size = band(index)
        rows = pl.ds(index * BLOCK, BLOCK)
        cols = pl.ds(start, size)
        place_q = lax.broadcasted_iota(jnp.int32, (BLOCK, size), 0) + (index * BLOCK - start)
        place_k = lax.broadcasted_iota(jnp.int32, (BLOCK, size), 1)
        allowed = (seg_col[rows, :] == seg_row[:, cols]) & (place_q >= place_k)
        query = q_ref[rows, :] * jnp.asarray(HD**-0.5, bf16)
        zero = jnp.zeros_like(query)
        keys = k_ref[cols, :]
        values = v_ref[cols, :]
        parts = []
        for head in range(2):
            mine = first if head == 0 else jnp.logical_not(first)
            scores = dot_nt(jnp.where(mine, query, zero), keys)
            scores = jnp.where(allowed, scores, masked_score)
            expon = jnp.exp(scores - jnp.max(scores, axis=-1, keepdims=True))
            total = jnp.sum(expon, axis=-1, keepdims=True)
            weights = (expon * (1.0 / total)).astype(bf16)
            prob_ref[head, rows, pl.ds(0, size)] = weights
            parts.append(dot(weights, values))
        out_ref[rows, :] = jnp.where(first, parts[0], parts[1]).astype(bf16)


def attn_forward(query, keys, values, seg_col, seg_row):
    length, width = query.shape
    pairs = width // (2 * HD)
    span = min(length, LONGEST + BLOCK)
    col = pl.BlockSpec((length, 2 * HD), lambda p: (0, p))
    return pl.pallas_call(
        attn_forward_kernel,
        grid=(pairs,),
        in_specs=[
            col,
            col,
            col,
            pl.BlockSpec((length, 1), lambda p: (0, 0)),
            pl.BlockSpec((1, length), lambda p: (0, 0)),
        ],
        out_specs=[col, pl.BlockSpec((2, length, span), lambda p: (p, 0, 0))],
        out_shape=[
            jax.ShapeDtypeStruct((length, width), bf16),
            jax.ShapeDtypeStruct((2 * pairs, length, span), bf16),
        ],
        compiler_params=pltpu.CompilerParams(vmem_limit_bytes=60 << 20),
        cost_estimate=pl.CostEstimate(
            flops=20 * 10**9, bytes_accessed=30 * 10**6, transcendentals=8 * 10**6
        ),
        name="attn_forward",
    )(query, keys, values, seg_col, seg_row)


def attn_backward_kernel(q_ref, k_ref, v_ref, grad_ref, prob_ref, gq_ref, gk_ref, gv_ref, gk, gv):
    length = q_ref.shape[0]
    first = lax.broadcasted_iota(jnp.int32, (BLOCK, 2 * HD), 1) < HD
    gk[...] = jnp.zeros_like(gk)
    gv[...] = jnp.zeros_like(gv)
    for index in range(length // BLOCK):
        start, size = band(index)
        rows = pl.ds(index * BLOCK, BLOCK)
        cols = pl.ds(start, size)
        query = q_ref[rows, :]
        grad = grad_ref[rows, :]
        keys = k_ref[cols, :]
        values = v_ref[cols, :]
        zero = jnp.zeros_like(query)
        parts = []
        for head in range(2):
            mine = first if head == 0 else jnp.logical_not(first)
            grad_head = jnp.where(mine, grad, zero)
            probs = prob_ref[head, rows, pl.ds(0, size)]
            grad_weights = dot_nt(grad_head, values)
            wide = probs.astype(f32)
            inner = jnp.sum(wide * grad_weights, axis=-1, keepdims=True)
            grad_scores = (wide * (grad_weights - inner)).astype(bf16)
            parts.append(dot(grad_scores, keys))
            gk[cols, :] += dot_tn(grad_scores, jnp.where(mine, query, zero))
            gv[cols, :] += dot_tn(probs, grad_head)
        gq_ref[rows, :] = (jnp.where(first, parts[0], parts[1]) * HD**-0.5).astype(bf16)
    gk_ref[...] = (gk[...] * HD**-0.5).astype(bf16)
    gv_ref[...] = gv[...].astype(bf16)


def attn_backward(query, keys, values, grad, probs):
    length, width = query.shape
    pairs = width // (2 * HD)
    span = probs.shape[-1]
    col = pl.BlockSpec((length, 2 * HD), lambda p: (0, p))
    shape = jax.ShapeDtypeStruct((length, width), bf16)
    return pl.pallas_call(
        attn_backward_kernel,
        grid=(pairs,),
        in_specs=[col, col, col, col, pl.BlockSpec((2, length, span), lambda p: (p, 0, 0))],
        out_specs=[col, col, col],
        out_shape=[shape, shape, shape],
        scratch_shapes=[pltpu.VMEM((length, 2 * HD), f32), pltpu.VMEM((length, 2 * HD), f32)],
        compiler_params=pltpu.CompilerParams(vmem_limit_bytes=60 << 20),
        cost_estimate=pl.CostEstimate(
            flops=50 * 10**9, bytes_accessed=30 * 10**6, transcendentals=0
        ),
        name="attn_backward",
    )(query, keys, values, grad, probs)


def expert_kernel(train, chunks, unread, *refs):
    refs = refs[:9] + refs[9 + unread :]
    inputs, outputs = refs[:9], refs[9 : 9 + (7 if train else 3)]
    scratch = refs[9 + len(outputs) :]
    normed, cot, share, pos_row, pos_col, up_block, up_b, down_block, down_b = inputs
    out_ref, gx_ref, gc_ref = outputs[:3]
    rows_x, rows_g, rows_out, rows_gx = scratch[:4]
    expert, chunk = pl.program_id(0), pl.program_id(1)
    last = chunks - 1
    length, width = normed.shape
    wide = up_block.shape[-1]
    up_w = up_block.reshape(width, wide)
    down_w = down_block.reshape(wide, width)

    if train:
        pack_ref, side_ref = outputs[5:]
        up_out, down_out, sems = scratch[4:]
        part = up_out.shape[1]
        group, tall = down_out.shape[:2]
        split = tall == (last + 1) * part
        final = pl.num_programs(0) - 1

        def each_copy(which_expert, which_chunk, act):
            base = which_expert * (2 * (last + 1) * part)
            up_at = pl.multiple_of(base + which_chunk * part, 8)
            shift = 0 if split else which_chunk * tall
            down_at = pl.multiple_of(base + (last + 1) * part + shift, 8)
            owners = pl.ds(which_chunk * group if split else 0, group)
            act(pltpu.make_async_copy(up_out, pack_ref.at[:, pl.ds(up_at, part), :], sems.at[0]))

            @pl.when(which_expert < final)
            def _():
                place = pack_ref.at[owners, pl.ds(down_at, tall), :]
                act(pltpu.make_async_copy(down_out, place, sems.at[1]))

            @pl.when(which_expert == final)
            def _():
                place = side_ref.at[owners, pl.ds(shift, tall), :]
                act(pltpu.make_async_copy(down_out, place, sems.at[1]))

    @pl.when((expert == 0) & (chunk == 0))
    def _():
        out_ref[...] = jnp.zeros_like(out_ref)
        gx_ref[...] = jnp.zeros_like(gx_ref)

    @pl.when(chunk == 0)
    def _():
        slots = lax.broadcasted_iota(jnp.int32, (CAP, length), 0)
        select = (slots == pos_row[0]).astype(bf16)
        rows_x[...] = dot(select, normed[...]).astype(bf16)
        scaled = (cot[...].astype(f32) * share[0]).astype(bf16)
        grads = dot(select, scaled)
        rows_g[...] = grads.astype(bf16)
        rows_out[...] = jnp.broadcast_to(down_b[0].astype(f32), rows_out.shape)
        rows_gx[...] = jnp.zeros_like(rows_gx)
        if train:
            outputs[4][0] = jnp.sum(grads, axis=0, keepdims=True)

    bias = up_b[0].astype(f32)

    up = dot(rows_x[...], up_w[...]) + bias
    back = dot_nt(rows_g[...], down_w[...])
    square = up * up
    bent = jnp.tanh(up * (0.7978845608028654 + (0.7978845608028654 * 0.044715) * square))
    half = 0.5 + 0.5 * bent
    active = (up * half).astype(bf16)
    slope = half + up * (half - half * bent) * (
        0.7978845608028654 + (3 * 0.044715 * 0.7978845608028654) * square
    )
    grad_up = (back * slope).astype(bf16)
    rows_out[...] += dot(active, down_w[...])
    rows_gx[...] += dot_nt(grad_up, up_w[...])
    if train:
        outputs[3][0] = jnp.sum(grad_up.astype(f32), axis=0, keepdims=True)
        previous = jnp.maximum(expert * (last + 1) + chunk - 1, 0)

        @pl.when((expert > 0) | (chunk > 0))
        def _():
            earlier = previous // (last + 1), lax.rem(previous, last + 1)
            each_copy(*earlier, lambda copy: copy.wait())

        up_out.reshape(width, wide)[...] = dot_tn(rows_x[...], grad_up).astype(bf16)
        down_out.reshape(wide, width)[...] = dot_tn(active, rows_g[...]).astype(bf16)
        each_copy(expert, chunk, lambda copy: copy.start())

        @pl.when((expert == final) & (chunk == last))
        def _():
            each_copy(expert, chunk, lambda copy: copy.wait())

    @pl.when(chunk == last)
    def _():
        slots = lax.broadcasted_iota(jnp.int32, (length, CAP), 1)
        select = (slots == pos_col[0]).astype(bf16)
        expert_out = dot(select, rows_out[...].astype(bf16))
        gc_ref[0] = jnp.sum(cot[...].astype(f32) * expert_out, axis=-1, keepdims=True)
        out_ref[...] += share[0] * expert_out
        gx_ref[...] += dot(select, rows_gx[...].astype(bf16))


def experts(
    train, normed, cot, share, pos_row, pos_col, up_w, down_w, up_b, down_b, behind=()
):
    length, width = normed.shape
    number, hidden = up_b.shape[0], up_b.shape[2]
    chunks = hidden // width
    whole = pl.BlockSpec((length, width), lambda e, j: (0, 0))
    column = pl.BlockSpec((1, length, 1), lambda e, j: (e, 0, 0))
    up_spec = pl.BlockSpec((width // up_w[1], up_w[1], width), up_w[2])
    down_spec = pl.BlockSpec((width // down_w[1], down_w[1], width), down_w[2])
    bias_spec = pl.BlockSpec((1, 1, width), lambda e, j: (e, 0, j))
    last_spec = pl.BlockSpec((1, 1, width), lambda e, j: (e, 0, 0))
    out_specs = [whole, whole, column]
    out_shape = [
        jax.ShapeDtypeStruct((length, width), f32),
        jax.ShapeDtypeStruct((length, width), f32),
        jax.ShapeDtypeStruct((number, length, 1), f32),
    ]
    scratch = [
        pltpu.VMEM((CAP, width), bf16),
        pltpu.VMEM((CAP, width), bf16),
        pltpu.VMEM((CAP, width), f32),
        pltpu.VMEM((CAP, width), f32),
    ]
    if train:
        part, tall = up_w[1], down_w[1]
        out_specs += [bias_spec, last_spec] + [pl.BlockSpec(memory_space=pl.ANY)] * 2
        out_shape += [
            jax.ShapeDtypeStruct(up_b.shape, f32),
            jax.ShapeDtypeStruct(down_b.shape, f32),
            jax.ShapeDtypeStruct((width // part, (2 * number - 1) * chunks * part, width), bf16),
            jax.ShapeDtypeStruct((width // part, chunks * part, width), bf16),
        ]
        scratch += [
            pltpu.VMEM((width // part, part, width), bf16),
            pltpu.VMEM((width // tall, tall, width), bf16),
            pltpu.SemaphoreType.DMA((2,)),
        ]
    return pl.pallas_call(
        functools.partial(expert_kernel, train, chunks, len(behind)),
        grid_spec=pltpu.PrefetchScalarGridSpec(
            num_scalar_prefetch=0,
            grid=(number, chunks),
            in_specs=[
                whole,
                whole,
                column,
                pl.BlockSpec((1, 1, length), lambda e, j: (e, 0, 0)),
                column,
                up_spec,
                bias_spec,
                down_spec,
                last_spec,
            ]
            + [pl.BlockSpec(memory_space=pl.ANY)] * len(behind),
            out_specs=out_specs,
            scratch_shapes=scratch,
        ),
        out_shape=out_shape,
        compiler_params=pltpu.CompilerParams(vmem_limit_bytes=60 << 20),
        cost_estimate=pl.CostEstimate(
            flops=(22 if train else 16) * number * 10**9,
            bytes_accessed=20 * number * 10**6,
            transcendentals=2 * number * 10**6,
        ),
        name="experts_new" if train else "experts_old",
    )(normed, cot, share, pos_row, pos_col, up_w[0], up_b, down_w[0], down_b, *behind)


def normalize(inputs):
    center = inputs - jnp.mean(inputs, axis=-1, keepdims=True)
    spread = jnp.mean(center * center, axis=-1, keepdims=True)
    scale = lax.rsqrt(spread + epsilon)
    return center * scale, scale


def normalize_back(unit, scale, grad):
    average = jnp.mean(grad, axis=-1, keepdims=True)
    along = jnp.mean(grad * unit, axis=-1, keepdims=True)
    return scale * (grad - average - unit * along)


def pack_experts(up, down):
    pieces = []
    width = down.shape[2]
    for expert in range(up.shape[0]):
        for start in range(0, up.shape[2], width):
            pieces.append(up[expert, :, start : start + width])
        pieces.append(down[expert])
    return pieces


def pack_small(shape, seven, router, new_ub, old_ub, new_db, old_db):
    places = ((seven, 0, 0), (router, 0, 128), (new_db, 4, 128), (old_db, 6, 128))
    places += ((new_ub, 0, 256), (old_ub, 2, 256))
    total = jnp.zeros(shape, bf16)
    for item, row, col in places:
        edges = ((row, shape[0] - row - item.shape[0]), (col, shape[1] - col - item.shape[1]))
        total = total + jnp.pad(item, edges)
    return total


def pack_kernel(new_up, new_down, old_up, old_down, w_q, w_k, w_v, small, new_out, old_out, a, b):
    for up, down, out in ((new_up, new_down, new_out), (old_up, old_down, old_out)):
        number, part, hidden = up.shape
        width = down.shape[2]
        at = 0
        for expert in range(number):
            for start in range(0, hidden, width):
                out[at : at + part, :] = up[expert, :, start : start + width]
                at += part
            out[at : at + down.shape[1], :] = down[expert]
            at += down.shape[1]
    part = w_q.shape[0]
    cut = a.shape[0] - part
    a[:part, :] = w_q[...]
    a[part:, :] = w_k[:cut, :]
    b[: part - cut, :] = w_k[cut:, :]
    b[part - cut : 2 * part - cut, :] = w_v[...]
    b[2 * part - cut :, :] = small[...]


def pack_all(new_up, new_down, old_up, old_down, w_query, w_key, w_value, small):
    part, width = w_query.shape
    if part % 8:
        new_pack = jnp.concatenate(pack_experts(new_up, new_down), axis=0)
        old_pack = jnp.concatenate(pack_experts(old_up, old_down), axis=0)
        head = jnp.concatenate([w_query, w_key, w_value, small], axis=0)
        middle = part + part // 2
        return new_pack, old_pack, head[:middle], head[middle:]
    rows = new_up.size // width + new_down.size // width
    half = (3 * part + 8) // 16 * 8
    shapes = [(rows, width), (rows, width), (half, width), (3 * part + 8 - half, width)]
    return pl.pallas_call(
        pack_kernel,
        out_shape=[jax.ShapeDtypeStruct(shape, bf16) for shape in shapes],
        name="pack",
    )(new_up, new_down, old_up, old_down, w_query, w_key, w_value, small)


def swap_of(name):
    if name == "narrow":
        return "narrow", lax.axis_index("narrow"), [(0, 1), (1, 0)]
    wide = lax.axis_size("wide")
    pairs = [(index, index ^ (1 << name)) for index in range(wide)]
    return "wide", (lax.axis_index("wide") >> name) & 1, pairs


def gather_all(mine, order):
    names = []
    held = mine
    for name in order:
        axis, bit, pairs = swap_of(name)
        got = lax.ppermute(held, axis, pairs)
        rank = -1 if name == "narrow" else name
        at = sum(1 for item in names if item > rank)
        names.insert(at, rank)
        low = jnp.stack([held, got], axis=at)
        high = jnp.stack([got, held], axis=at)
        held = jnp.where(bit == 0, low, high)
    return held.reshape((-1,) + mine.shape)


def expert_blocks(gathered, number, part, chunks):
    count, width = gathered.shape[0], gathered.shape[2]
    if part % 8 == 0:
        up = (gathered, part, lambda e, j: (0, 2 * chunks * e + j, 0))
        down = (gathered, chunks * part, lambda e, j: (j, 2 * e + 1, 0))
        return up, down
    both = gathered[:, : number * 2 * chunks * part].reshape(count, number, 2, -1, width)
    tall = both[:, :, 0].reshape(count, number, chunks, part, width).transpose(1, 2, 0, 3, 4)
    tall = tall.reshape(1, number * chunks * width, width)
    flat = both[:, :, 1].transpose(1, 0, 2, 3).reshape(1, number * chunks * width, width)
    place = lambda e, j: (0, chunks * e + j, 0)
    return (tall, width, place), (flat, width, place)


def split_blocks(up, down, part, chunks):
    if part % 8 == 0:
        return (up, part, lambda e, j: (0, j, 0)), (down, chunks * part, lambda e, j: (j, 0, 0))
    return expert_blocks(jnp.concatenate([up, down], axis=1), 1, part, chunks)


def by_owner(packed, side, number, part, chunks):
    if part % 8 == 0:
        return packed, side
    width = packed.shape[2]
    count = width // part
    both = jnp.concatenate([packed, side], axis=1).reshape(number, 2, chunks, width, width)
    up = both[:, 0].reshape(number, chunks, count, part, width).transpose(2, 0, 1, 3, 4)
    down = both[:, 1].reshape(number, count, chunks, part, width).transpose(1, 0, 2, 3, 4)
    whole = jnp.stack([up, down], axis=2).reshape(count, -1, width)
    return whole[:, : -chunks * part], whole[:, -chunks * part :]


def scatter_sum(parts, order):
    bits = lax.axis_size("wide").bit_length() - 1
    names = list(range(bits - 1, -1, -1)) + ["narrow"]
    parts = parts.reshape((2,) * len(names) + parts.shape[1:])
    for name in order:
        at = names.index(name)
        names.pop(at)
        axis, mine, swap = swap_of(name)
        sent = lax.dynamic_index_in_dim(parts, 1 - mine, at, keepdims=False)
        kept = lax.dynamic_index_in_dim(parts, mine, at, keepdims=False)
        got = lax.ppermute(sent, axis, swap)
        parts = (kept.astype(f32) + got.astype(f32)).astype(bf16)
    return parts


def local(
    tokens,
    cotangent,
    segment_ids,
    routes,
    replay,
    gain_one,
    shift_one,
    w_query,
    b_query,
    w_key,
    w_value,
    b_value,
    w_out,
    b_out,
    gain_two,
    shift_two,
    w_router,
    new_up,
    new_up_bias,
    new_down,
    new_down_bias,
    old_up,
    old_up_bias,
    old_down,
    old_down_bias,
):
    seqs_here, length, width = tokens.shape
    part = w_query.shape[0]
    count = width // part
    hidden = new_up.shape[-1]
    new_count = new_up.shape[0]

    chunks = hidden // width
    bits = list(range(2, lax.axis_size("wide").bit_length() - 1))
    one_way = [0, 1, "narrow"] + bits
    other_way = [0, "narrow", 1] + bits

    seven = jnp.stack([gain_one, shift_one, b_query, b_value, b_out, gain_two, shift_two])
    small = pack_small(
        (8, width),
        seven,
        w_router.T,
        new_up_bias,
        old_up_bias,
        new_down_bias,
        old_down_bias,
    )
    new_pack, old_pack, head_a, head_b = pack_all(
        new_up, new_down, old_up, old_down, w_query, w_key, w_value, small
    )
    new_all = lax.all_gather(new_pack, AXES, axis=0)
    old_all = lax.all_gather(old_pack, AXES, axis=0)
    all_a = gather_all(head_a, one_way[::-1])
    all_b = gather_all(head_b, other_way[::-1])
    full_out = gather_all(w_out, one_way[::-1]).reshape(width, width)
    cut = head_a.shape[0] - part
    full_query = all_a[:, :part].reshape(width, width)
    full_key = jnp.concatenate([all_a[:, part:], all_b[:, : part - cut]], axis=1)
    full_key = full_key.reshape(width, width)
    full_value = all_b[:, part - cut : 2 * part - cut].reshape(width, width)
    block = all_b[:, 2 * part - cut :]

    def columns(row, rows, col, wide):
        return block[:, row : row + rows, col : col + wide].transpose(1, 0, 2).reshape(rows, -1)

    seven = columns(0, 7, 0, part).astype(f32)
    gain_first, shift_first, bias_q, bias_v, bias_o, gain_second, shift_second = seven
    router = columns(0, EXPERTS, 128, part).T
    new_down_b = columns(4, new_count, 128, part)[:, None, :]
    old_down_b = columns(6, new_count, 128, part)[:, None, :]
    new_up_b = columns(0, new_count, 256, new_up_bias.shape[1])[:, None, :]
    old_up_b = columns(2, new_count, 256, new_up_bias.shape[1])[:, None, :]

    flat = tokens.reshape(length, width).astype(f32)
    cot = cotangent.reshape(length, width)
    segments = segment_ids.reshape(length)
    route_flat = routes.reshape(length, -1)
    member = jnp.any(
        route_flat[:, :, None] == jnp.arange(EXPERTS, dtype=jnp.int32)[None, None, :], axis=1
    )
    member_int = member.astype(jnp.int32)
    running = jnp.cumsum(member_int, axis=0)
    position = jnp.where(member, running - 1, -1)
    pos_row = position.T[:, None, :]
    pos_col = position.T[:, :, None]

    unit_one, scale_one = normalize(flat)
    normed = (unit_one * gain_first + shift_first).astype(bf16)
    query = (dot(normed, full_query) + bias_q).astype(bf16)
    keys = dot(normed, full_key).astype(bf16)
    values = (dot(normed, full_value) + bias_v).astype(bf16)
    mixed, probs = attn_forward(query, keys, values, segments[:, None], segments[None, :])
    resid = flat + dot(mixed, full_out) + bias_o
    unit_two, scale_two = normalize(resid)
    normed_two = (unit_two * gain_second + shift_second).astype(bf16)
    logits = dot(normed_two, router)
    trained = (jnp.arange(EXPERTS) >= FROZEN).astype(f32)
    keep = 1.0 - replay.reshape(length, 1).astype(f32) * trained

    def gate_map(values_in):
        gate = jax.nn.softmax(values_in, axis=-1)
        picked = jnp.where(member, gate, 0.0)
        return picked / jnp.sum(picked, axis=-1, keepdims=True) * keep

    share, gate_back = jax.vjp(gate_map, logits)
    share_cols = share.T[:, :, None]

    got = experts(
        True,
        normed_two,
        cot,
        share_cols[FROZEN:],
        pos_row[FROZEN:],
        pos_col[FROZEN:],
        *expert_blocks(new_all, new_count, part, chunks),
        new_up_b,
        new_down_b,
    )
    out_new, gx_new, gc_new, grad_up_b, grad_down_b, packed, side = got
    packed, side = by_owner(packed, side, new_count, part, chunks)
    tall = chunks * part
    summed_new = lax.psum_scatter(
        packed.reshape(-1, width), AXES, scatter_dimension=0, tiled=True
    ).astype(f32)
    middle = tall // 2
    side_sums = [
        scatter_sum(side[:, :middle], one_way),
        scatter_sum(side[:, middle:], other_way),
    ]
    side_sum = jnp.concatenate(side_sums, axis=0).astype(f32)
    sum_up = jnp.stack([summed_new[:tall], summed_new[2 * tall :]])
    sum_up = sum_up.reshape(new_count, chunks, part, width).transpose(0, 2, 1, 3)
    sum_up = sum_up.reshape(new_count, part, hidden)
    sum_down = jnp.stack([summed_new[tall : 2 * tall], side_sum])

    out_old, gx_old, gc_old = experts(
        False,
        normed_two,
        cot,
        share_cols[:FROZEN],
        pos_row[:FROZEN],
        pos_col[:FROZEN],
        *expert_blocks(old_all, old_up.shape[0], part, chunks),
        old_up_b,
        old_down_b,
        behind=(side_sum,),
    )
    result = (resid + out_new + out_old).astype(bf16)
    grad_share = jnp.concatenate([gc_old, gc_new], axis=0)[:, :, 0].T
    grad_logits = gate_back(grad_share)[0]
    grad_router = lax.dot_general(
        normed_two.astype(f32),
        grad_logits,
        (((0,), (0,)), ((), ())),
        precision=lax.Precision.HIGHEST,
        preferred_element_type=f32,
    )
    grad_two = gx_new + gx_old
    for expert in range(EXPERTS):
        grad_two = grad_two + grad_logits[:, expert : expert + 1] * router[:, expert].astype(f32)
    grad_two = grad_two.astype(bf16).astype(f32)
    grad_gain_two = jnp.sum(grad_two * unit_two, axis=0)
    grad_shift_two = jnp.sum(grad_two, axis=0)
    grad_resid = cot.astype(f32) + normalize_back(unit_two, scale_two, grad_two * gain_second)
    grad_attn = grad_resid.astype(bf16)
    grad_w_out = dot_tn(mixed, grad_attn)
    grad_b_out = jnp.sum(grad_attn.astype(f32), axis=0)
    grad_w_out = grad_w_out.reshape(count, part, width).astype(bf16)
    grad_w_out, grad_attn = lax.optimization_barrier((grad_w_out, grad_attn))
    grad_mixed = dot_nt(grad_attn, full_out).astype(bf16)
    grad_q, grad_k, grad_v = attn_backward(query, keys, values, grad_mixed, probs)
    grad_w_query = dot_tn(normed, grad_q)
    grad_w_key = dot_tn(normed, grad_k)
    grad_w_value = dot_tn(normed, grad_v)
    pieces = [
        item.reshape(count, part, width).astype(bf16)
        for item in (grad_w_query, grad_w_key, grad_w_value)
    ]
    last_a = jnp.concatenate([pieces[0], grad_w_out], axis=1)
    last_b = jnp.concatenate(pieces[1:], axis=1)
    last_a, last_b, grad_q, grad_k, grad_v = lax.optimization_barrier(
        (last_a, last_b, grad_q, grad_k, grad_v)
    )
    sum_a = scatter_sum(last_a, one_way).astype(f32)
    grad_b_query = jnp.sum(grad_q.astype(f32), axis=0)
    grad_b_value = jnp.sum(grad_v.astype(f32), axis=0)
    grad_one = dot_nt(grad_q, full_query) + dot_nt(grad_k, full_key) + dot_nt(grad_v, full_value)
    grad_one = grad_one.astype(bf16).astype(f32)
    grad_gain_one = jnp.sum(grad_one * unit_one, axis=0)
    grad_shift_one = jnp.sum(grad_one, axis=0)
    grad_input = grad_resid + normalize_back(unit_one, scale_one, grad_one * gain_first)

    vectors = [grad_gain_one, grad_shift_one, grad_b_query, grad_b_value, grad_b_out]
    vectors += [grad_gain_two, grad_shift_two, grad_router]
    rows = [item.reshape(count, -1) for item in vectors]
    for item in (grad_up_b, grad_down_b):
        rows.append(item.reshape(new_count, count, -1).transpose(1, 0, 2).reshape(count, -1))
    lengths = [item.shape[1] for item in rows]
    row = jnp.concatenate(rows, axis=1).astype(bf16)
    row = jnp.pad(row, ((0, 0), (0, 8 * width - row.shape[1]))).reshape(count, 8, width)
    sum_b = scatter_sum(jnp.concatenate([last_b, row], axis=1), other_way).astype(f32)
    sums = [sum_a[:part], sum_b[:part], sum_b[part : 2 * part], sum_a[part:]]
    tail = sum_b[2 * part]
    found = []
    at = 0
    for size in lengths:
        found.append(tail[at : at + size])
        at += size
    return (
        result.reshape(seqs_here, length, width),
        grad_input.astype(bf16).reshape(seqs_here, length, width),
        found[0],
        found[1],
        sums[0],
        found[2],
        sums[1],
        sums[2],
        found[3],
        sums[3],
        found[4],
        found[5],
        found[6],
        found[7].reshape(part, EXPERTS),
        sum_up,
        found[8].reshape(new_count, -1),
        sum_down,
        found[9].reshape(new_count, -1),
    )


def solution(mesh):
    axes = AXES
    rows3 = P(axes, None, None)
    rows2 = P(axes, None)
    rows1 = P(axes)
    mid3 = P(None, axes, None)
    mid2 = P(None, axes)
    placed = (rows3, rows3, rows2, rows3, rows2)
    placed += (rows1, rows1, rows2, rows1, rows2, rows2, rows1, rows2, rows1, rows1, rows1, rows2)
    placed += (mid3, mid2) * 4
    outs = (rows3, rows3, rows1, rows1, rows2, rows1, rows2, rows2, rows1, rows2, rows1)
    outs += (rows1, rows1, rows2, mid3, mid2, mid3, mid2)
    return jax.shard_map(local, mesh=mesh, in_specs=placed, out_specs=outs, check_vma=False)
```

```python
import functools

import jax
import jax.numpy as jnp
from jax import lax
from jax.experimental import pallas as pl
from jax.experimental.pallas import tpu as pltpu
from jax.sharding import PartitionSpec as P

HD = 64
FROZEN = 2
EXPERTS = 4
CAP = 640
BLOCK = 256
LONGEST = 512
AXES = ("wide", "narrow")

epsilon = 1e-05
masked_score = -1e30
f32 = jnp.float32
bf16 = jnp.bfloat16


def dot(a, b):
    return jnp.dot(a, b, preferred_element_type=f32)


def dot_nt(a, b):
    return lax.dot_general(a, b, (((1,), (1,)), ((), ())), preferred_element_type=f32)


def dot_tn(a, b):
    return lax.dot_general(a, b, (((0,), (0,)), ((), ())), preferred_element_type=f32)


def band(index):
    start = max(0, index - LONGEST // BLOCK) * BLOCK
    return start, (index + 1) * BLOCK - start


def attn_forward_kernel(q_ref, k_ref, v_ref, seg_col, seg_row, out_ref, prob_ref):
    length = q_ref.shape[0]
    first = lax.broadcasted_iota(jnp.int32, (BLOCK, 2 * HD), 1) < HD
    for index in range(length // BLOCK):
        start, size = band(index)
        rows = pl.ds(index * BLOCK, BLOCK)
        cols = pl.ds(start, size)
        place_q = lax.broadcasted_iota(jnp.int32, (BLOCK, size), 0) + (index * BLOCK - start)
        place_k = lax.broadcasted_iota(jnp.int32, (BLOCK, size), 1)
        allowed = (seg_col[rows, :] == seg_row[:, cols]) & (place_q >= place_k)
        query = q_ref[rows, :] * jnp.asarray(HD**-0.5, bf16)
        zero = jnp.zeros_like(query)
        keys = k_ref[cols, :]
        values = v_ref[cols, :]
        parts = []
        for head in range(2):
            mine = first if head == 0 else jnp.logical_not(first)
            scores = dot_nt(jnp.where(mine, query, zero), keys)
            scores = jnp.where(allowed, scores, masked_score)
            expon = jnp.exp(scores - jnp.max(scores, axis=-1, keepdims=True))
            total = jnp.sum(expon, axis=-1, keepdims=True)
            weights = (expon * (1.0 / total)).astype(bf16)
            prob_ref[head, rows, pl.ds(0, size)] = weights
            parts.append(dot(weights, values))
        out_ref[rows, :] = jnp.where(first, parts[0], parts[1]).astype(bf16)


def attn_forward(query, keys, values, seg_col, seg_row):
    length, width = query.shape
    pairs = width // (2 * HD)
    span = min(length, LONGEST + BLOCK)
    col = pl.BlockSpec((length, 2 * HD), lambda p: (0, p))
    return pl.pallas_call(
        attn_forward_kernel,
        grid=(pairs,),
        in_specs=[
            col,
            col,
            col,
            pl.BlockSpec((length, 1), lambda p: (0, 0)),
            pl.BlockSpec((1, length), lambda p: (0, 0)),
        ],
        out_specs=[col, pl.BlockSpec((2, length, span), lambda p: (p, 0, 0))],
        out_shape=[
            jax.ShapeDtypeStruct((length, width), bf16),
            jax.ShapeDtypeStruct((2 * pairs, length, span), bf16),
        ],
        compiler_params=pltpu.CompilerParams(vmem_limit_bytes=60 << 20),
        cost_estimate=pl.CostEstimate(
            flops=20 * 10**9, bytes_accessed=30 * 10**6, transcendentals=8 * 10**6
        ),
        name="attn_forward",
    )(query, keys, values, seg_col, seg_row)


def attn_backward_kernel(*refs):
    q_ref, k_ref, v_ref, grad_ref, prob_ref = refs[:5]
    gq_ref, gk_ref, gv_ref, gk, gv = refs[-5:]
    length = q_ref.shape[0]
    first = lax.broadcasted_iota(jnp.int32, (BLOCK, 2 * HD), 1) < HD
    gk[...] = jnp.zeros_like(gk)
    gv[...] = jnp.zeros_like(gv)
    for index in range(length // BLOCK):
        start, size = band(index)
        rows = pl.ds(index * BLOCK, BLOCK)
        cols = pl.ds(start, size)
        query = q_ref[rows, :]
        grad = grad_ref[rows, :]
        keys = k_ref[cols, :]
        values = v_ref[cols, :]
        zero = jnp.zeros_like(query)
        parts = []
        for head in range(2):
            mine = first if head == 0 else jnp.logical_not(first)
            grad_head = jnp.where(mine, grad, zero)
            probs = prob_ref[head, rows, pl.ds(0, size)]
            grad_weights = dot_nt(grad_head, values)
            wide = probs.astype(f32)
            inner = jnp.sum(wide * grad_weights, axis=-1, keepdims=True)
            grad_scores = (wide * (grad_weights - inner)).astype(bf16)
            parts.append(dot(grad_scores, keys))
            gk[cols, :] += dot_tn(grad_scores, jnp.where(mine, query, zero))
            gv[cols, :] += dot_tn(probs, grad_head)
        gq_ref[rows, :] = (jnp.where(first, parts[0], parts[1]) * HD**-0.5).astype(bf16)
    gk_ref[...] = (gk[...] * HD**-0.5).astype(bf16)
    gv_ref[...] = gv[...].astype(bf16)


def attn_backward(query, keys, values, grad, probs, behind):
    length, width = query.shape
    pairs = width // (2 * HD)
    span = probs.shape[-1]
    col = pl.BlockSpec((length, 2 * HD), lambda p: (0, p))
    shape = jax.ShapeDtypeStruct((length, width), bf16)
    return pl.pallas_call(
        attn_backward_kernel,
        grid=(pairs,),
        in_specs=[col, col, col, col, pl.BlockSpec((2, length, span), lambda p: (p, 0, 0))]
        + [pl.BlockSpec(memory_space=pl.ANY)] * len(behind),
        out_specs=[col, col, col],
        out_shape=[shape, shape, shape],
        scratch_shapes=[pltpu.VMEM((length, 2 * HD), f32), pltpu.VMEM((length, 2 * HD), f32)],
        compiler_params=pltpu.CompilerParams(vmem_limit_bytes=60 << 20),
        cost_estimate=pl.CostEstimate(
            flops=50 * 10**9, bytes_accessed=30 * 10**6, transcendentals=0
        ),
        name="attn_backward",
    )(query, keys, values, grad, probs, *behind)


def expert_kernel(train, chunks, unread, *refs):
    refs = refs[:9] + refs[9 + unread :]
    inputs, outputs = refs[:9], refs[9 : 9 + (7 if train else 3)]
    scratch = refs[9 + len(outputs) :]
    normed, cot, share, pos_row, pos_col, up_block, up_b, down_block, down_b = inputs
    out_ref, gx_ref, gc_ref = outputs[:3]
    rows_x, rows_g, rows_out, rows_gx = scratch[:4]
    expert, chunk = pl.program_id(0), pl.program_id(1)
    last = chunks - 1
    length, width = normed.shape
    wide = up_block.shape[-1]
    up_w = up_block.reshape(width, wide)
    down_w = down_block.reshape(wide, width)

    if train:
        pack_ref, side_ref = outputs[5:]
        up_out, down_out, sems = scratch[4:]
        part = up_out.shape[1]
        group, tall = down_out.shape[:2]
        split = tall == (last + 1) * part
        final = pl.num_programs(0) - 1

        def each_copy(which_expert, which_chunk, act):
            base = which_expert * (2 * (last + 1) * part)
            up_at = pl.multiple_of(base + which_chunk * part, 8)
            shift = 0 if split else which_chunk * tall
            down_at = pl.multiple_of(base + (last + 1) * part + shift, 8)
            owners = pl.ds(which_chunk * group if split else 0, group)
            act(pltpu.make_async_copy(up_out, pack_ref.at[:, pl.ds(up_at, part), :], sems.at[0]))

            @pl.when(which_expert < final)
            def _():
                place = pack_ref.at[owners, pl.ds(down_at, tall), :]
                act(pltpu.make_async_copy(down_out, place, sems.at[1]))

            @pl.when(which_expert == final)
            def _():
                place = side_ref.at[owners, pl.ds(shift, tall), :]
                act(pltpu.make_async_copy(down_out, place, sems.at[1]))

    @pl.when((expert == 0) & (chunk == 0))
    def _():
        out_ref[...] = jnp.zeros_like(out_ref)
        gx_ref[...] = jnp.zeros_like(gx_ref)

    @pl.when(chunk == 0)
    def _():
        slots = lax.broadcasted_iota(jnp.int32, (CAP, length), 0)
        select = (slots == pos_row[0]).astype(bf16)
        rows_x[...] = dot(select, normed[...]).astype(bf16)
        scaled = (cot[...].astype(f32) * share[0]).astype(bf16)
        grads = dot(select, scaled)
        rows_g[...] = grads.astype(bf16)
        rows_out[...] = jnp.broadcast_to(down_b[0].astype(f32), rows_out.shape)
        rows_gx[...] = jnp.zeros_like(rows_gx)
        if train:
            outputs[4][0] = jnp.sum(grads, axis=0, keepdims=True)

    bias = up_b[0].astype(f32)

    up = dot(rows_x[...], up_w[...]) + bias
    back = dot_nt(rows_g[...], down_w[...])
    square = up * up
    bent = jnp.tanh(up * (0.7978845608028654 + (0.7978845608028654 * 0.044715) * square))
    half = 0.5 + 0.5 * bent
    active = (up * half).astype(bf16)
    slope = half + up * (half - half * bent) * (
        0.7978845608028654 + (3 * 0.044715 * 0.7978845608028654) * square
    )
    grad_up = (back * slope).astype(bf16)
    rows_out[...] += dot(active, down_w[...])
    rows_gx[...] += dot_nt(grad_up, up_w[...])
    if train:
        outputs[3][0] = jnp.sum(grad_up.astype(f32), axis=0, keepdims=True)
        previous = jnp.maximum(expert * (last + 1) + chunk - 1, 0)

        @pl.when((expert > 0) | (chunk > 0))
        def _():
            earlier = previous // (last + 1), lax.rem(previous, last + 1)
            each_copy(*earlier, lambda copy: copy.wait())

        up_out.reshape(width, wide)[...] = dot_tn(rows_x[...], grad_up).astype(bf16)
        down_out.reshape(wide, width)[...] = dot_tn(active, rows_g[...]).astype(bf16)
        each_copy(expert, chunk, lambda copy: copy.start())

        @pl.when((expert == final) & (chunk == last))
        def _():
            each_copy(expert, chunk, lambda copy: copy.wait())

    @pl.when(chunk == last)
    def _():
        slots = lax.broadcasted_iota(jnp.int32, (length, CAP), 1)
        select = (slots == pos_col[0]).astype(bf16)
        expert_out = dot(select, rows_out[...].astype(bf16))
        gc_ref[0] = jnp.sum(cot[...].astype(f32) * expert_out, axis=-1, keepdims=True)
        out_ref[...] += share[0] * expert_out
        gx_ref[...] += dot(select, rows_gx[...].astype(bf16))


def experts(
    train, normed, cot, share, pos_row, pos_col, up_w, down_w, up_b, down_b, behind=()
):
    length, width = normed.shape
    number, hidden = up_b.shape[0], up_b.shape[2]
    chunks = hidden // width
    whole = pl.BlockSpec((length, width), lambda e, j: (0, 0))
    column = pl.BlockSpec((1, length, 1), lambda e, j: (e, 0, 0))
    up_spec = pl.BlockSpec((width // up_w[1], up_w[1], width), up_w[2])
    down_spec = pl.BlockSpec((width // down_w[1], down_w[1], width), down_w[2])
    bias_spec = pl.BlockSpec((1, 1, width), lambda e, j: (e, 0, j))
    last_spec = pl.BlockSpec((1, 1, width), lambda e, j: (e, 0, 0))
    out_specs = [whole, whole, column]
    out_shape = [
        jax.ShapeDtypeStruct((length, width), f32),
        jax.ShapeDtypeStruct((length, width), f32),
        jax.ShapeDtypeStruct((number, length, 1), f32),
    ]
    scratch = [
        pltpu.VMEM((CAP, width), bf16),
        pltpu.VMEM((CAP, width), bf16),
        pltpu.VMEM((CAP, width), f32),
        pltpu.VMEM((CAP, width), f32),
    ]
    if train:
        part, tall = up_w[1], down_w[1]
        out_specs += [bias_spec, last_spec] + [pl.BlockSpec(memory_space=pl.ANY)] * 2
        out_shape += [
            jax.ShapeDtypeStruct(up_b.shape, f32),
            jax.ShapeDtypeStruct(down_b.shape, f32),
            jax.ShapeDtypeStruct((width // part, (2 * number - 1) * chunks * part, width), bf16),
            jax.ShapeDtypeStruct((width // part, chunks * part, width), bf16),
        ]
        scratch += [
            pltpu.VMEM((width // part, part, width), bf16),
            pltpu.VMEM((width // tall, tall, width), bf16),
            pltpu.SemaphoreType.DMA((2,)),
        ]
    return pl.pallas_call(
        functools.partial(expert_kernel, train, chunks, len(behind)),
        grid_spec=pltpu.PrefetchScalarGridSpec(
            num_scalar_prefetch=0,
            grid=(number, chunks),
            in_specs=[
                whole,
                whole,
                column,
                pl.BlockSpec((1, 1, length), lambda e, j: (e, 0, 0)),
                column,
                up_spec,
                bias_spec,
                down_spec,
                last_spec,
            ]
            + [pl.BlockSpec(memory_space=pl.ANY)] * len(behind),
            out_specs=out_specs,
            scratch_shapes=scratch,
        ),
        out_shape=out_shape,
        compiler_params=pltpu.CompilerParams(vmem_limit_bytes=60 << 20),
        cost_estimate=pl.CostEstimate(
            flops=(22 if train else 16) * number * 10**9,
            bytes_accessed=20 * number * 10**6,
            transcendentals=2 * number * 10**6,
        ),
        name="experts_new" if train else "experts_old",
    )(normed, cot, share, pos_row, pos_col, up_w[0], up_b, down_w[0], down_b, *behind)


def normalize(inputs):
    center = inputs - jnp.mean(inputs, axis=-1, keepdims=True)
    spread = jnp.mean(center * center, axis=-1, keepdims=True)
    scale = lax.rsqrt(spread + epsilon)
    return center * scale, scale


def normalize_back(unit, scale, grad):
    average = jnp.mean(grad, axis=-1, keepdims=True)
    along = jnp.mean(grad * unit, axis=-1, keepdims=True)
    return scale * (grad - average - unit * along)


def pack_experts(up, down):
    pieces = []
    width = down.shape[2]
    for expert in range(up.shape[0]):
        for start in range(0, up.shape[2], width):
            pieces.append(up[expert, :, start : start + width])
        pieces.append(down[expert])
    return pieces


def pack_small(shape, seven, router, new_ub, old_ub, new_db, old_db):
    places = ((seven, 0, 0), (router, 0, 128), (new_db, 4, 128), (old_db, 6, 128))
    places += ((new_ub, 0, 256), (old_ub, 2, 256))
    total = jnp.zeros(shape, bf16)
    for item, row, col in places:
        edges = ((row, shape[0] - row - item.shape[0]), (col, shape[1] - col - item.shape[1]))
        total = total + jnp.pad(item, edges)
    return total


def pack_kernel(new_up, new_down, old_up, old_down, w_q, w_k, w_v, small, new_out, old_out, a, b):
    width = new_down.shape[2]
    pairs = [(new_up, new_down, expert) for expert in range(new_up.shape[0])]
    pairs.append((old_up, old_down, 0))
    at = 0
    for up, down, expert in pairs + [(old_up, old_down, 1)]:
        out, at = (old_out, 0) if at == new_out.shape[0] else (new_out, at)
        for start in range(0, up.shape[2], width):
            out[at : at + up.shape[1], :] = up[expert, :, start : start + width]
            at += up.shape[1]
        out[at : at + down.shape[1], :] = down[expert]
        at += down.shape[1]
    part = w_q.shape[0]
    cut = a.shape[0] - part
    a[:part, :] = w_q[...]
    a[part:, :] = w_k[:cut, :]
    b[: part - cut, :] = w_k[cut:, :]
    b[part - cut : 2 * part - cut, :] = w_v[...]
    b[2 * part - cut :, :] = small[...]


def pack_all(new_up, new_down, old_up, old_down, w_query, w_key, w_value, small):
    part, width = w_query.shape
    if part % 8:
        lead = pack_experts(new_up, new_down) + pack_experts(old_up[:1], old_down[:1])
        new_pack = jnp.concatenate(lead, axis=0)
        old_pack = jnp.concatenate(pack_experts(old_up[1:], old_down[1:]), axis=0)
        head = jnp.concatenate([w_query, w_key, w_value, small], axis=0)
        middle = part + part // 2
        return new_pack, old_pack, head[:middle], head[middle:]
    rows = old_up[0].size // width + old_down[0].size // width
    half = (3 * part + 8) // 16 * 8
    shapes = [(3 * rows, width), (rows, width), (half, width), (3 * part + 8 - half, width)]
    return pl.pallas_call(
        pack_kernel,
        out_shape=[jax.ShapeDtypeStruct(shape, bf16) for shape in shapes],
        name="pack",
    )(new_up, new_down, old_up, old_down, w_query, w_key, w_value, small)


def swap_of(name):
    if name == "narrow":
        return "narrow", lax.axis_index("narrow"), [(0, 1), (1, 0)]
    wide = lax.axis_size("wide")
    pairs = [(index, index ^ (1 << name)) for index in range(wide)]
    return "wide", (lax.axis_index("wide") >> name) & 1, pairs


def gather_all(mine, order):
    names = []
    held = mine
    for name in order:
        axis, bit, pairs = swap_of(name)
        got = lax.ppermute(held, axis, pairs)
        rank = -1 if name == "narrow" else name
        at = sum(1 for item in names if item > rank)
        names.insert(at, rank)
        low = jnp.stack([held, got], axis=at)
        high = jnp.stack([got, held], axis=at)
        held = jnp.where(bit == 0, low, high)
    return held.reshape((-1,) + mine.shape)


def expert_blocks(gathered, skip, number, part, chunks):
    count, width = gathered.shape[0], gathered.shape[2]
    if part % 8 == 0:
        up = (gathered, part, lambda e, j: (0, 2 * chunks * (e + skip) + j, 0))
        down = (gathered, chunks * part, lambda e, j: (j, 2 * (e + skip) + 1, 0))
        return up, down
    rows = 2 * chunks * part
    both = gathered[:, skip * rows : (skip + number) * rows]
    both = both.reshape(count, number, 2, -1, width)
    tall = both[:, :, 0].reshape(count, number, chunks, part, width).transpose(1, 2, 0, 3, 4)
    tall = tall.reshape(1, number * chunks * width, width)
    flat = both[:, :, 1].transpose(1, 0, 2, 3).reshape(1, number * chunks * width, width)
    place = lambda e, j: (0, chunks * e + j, 0)
    return (tall, width, place), (flat, width, place)


def split_blocks(up, down, part, chunks):
    if part % 8 == 0:
        return (up, part, lambda e, j: (0, j, 0)), (down, chunks * part, lambda e, j: (j, 0, 0))
    return expert_blocks(jnp.concatenate([up, down], axis=1), 1, part, chunks)


def by_owner(packed, side, number, part, chunks):
    if part % 8 == 0:
        return packed, side
    width = packed.shape[2]
    count = width // part
    both = jnp.concatenate([packed, side], axis=1).reshape(number, 2, chunks, width, width)
    up = both[:, 0].reshape(number, chunks, count, part, width).transpose(2, 0, 1, 3, 4)
    down = both[:, 1].reshape(number, count, chunks, part, width).transpose(1, 0, 2, 3, 4)
    whole = jnp.stack([up, down], axis=2).reshape(count, -1, width)
    return whole[:, : -chunks * part], whole[:, -chunks * part :]


def scatter_sum(parts, order, partial=None):
    bits = lax.axis_size("wide").bit_length() - 1
    names = list(range(bits - 1, -1, -1)) + ["narrow"]
    parts = parts.reshape((2,) * len(names) + parts.shape[1:])
    for name in order:
        at = names.index(name)
        names.pop(at)
        axis, mine, swap = swap_of(name)
        sent = lax.dynamic_index_in_dim(parts, 1 - mine, at, keepdims=False)
        kept = lax.dynamic_index_in_dim(parts, mine, at, keepdims=False)
        got = lax.ppermute(sent, axis, swap)
        parts = (kept.astype(f32) + got.astype(f32)).astype(bf16)
        if partial is not None:
            partial.append(parts)
    return parts


def local(
    tokens,
    cotangent,
    segment_ids,
    routes,
    replay,
    gain_one,
    shift_one,
    w_query,
    b_query,
    w_key,
    w_value,
    b_value,
    w_out,
    b_out,
    gain_two,
    shift_two,
    w_router,
    new_up,
    new_up_bias,
    new_down,
    new_down_bias,
    old_up,
    old_up_bias,
    old_down,
    old_down_bias,
):
    seqs_here, length, width = tokens.shape
    part = w_query.shape[0]
    count = width // part
    hidden = new_up.shape[-1]
    new_count = new_up.shape[0]

    chunks = hidden // width
    bits = list(range(2, lax.axis_size("wide").bit_length() - 1))
    one_way = [0, 1, "narrow"] + bits
    other_way = [0, "narrow", 1] + bits

    seven = jnp.stack([gain_one, shift_one, b_query, b_value, b_out, gain_two, shift_two])
    small = pack_small(
        (8, width),
        seven,
        w_router.T,
        new_up_bias,
        old_up_bias,
        new_down_bias,
        old_down_bias,
    )
    new_pack, old_pack, head_a, head_b = pack_all(
        new_up, new_down, old_up, old_down, w_query, w_key, w_value, small
    )
    new_all = lax.all_gather(new_pack, AXES, axis=0)
    old_all = lax.all_gather(old_pack, AXES, axis=0)
    all_a = gather_all(head_a, one_way[::-1])
    all_b = gather_all(head_b, other_way[::-1])
    full_out = gather_all(w_out, one_way[::-1]).reshape(width, width)
    cut = head_a.shape[0] - part
    full_query = all_a[:, :part].reshape(width, width)
    full_key = jnp.concatenate([all_a[:, part:], all_b[:, : part - cut]], axis=1)
    full_key = full_key.reshape(width, width)
    full_value = all_b[:, part - cut : 2 * part - cut].reshape(width, width)
    block = all_b[:, 2 * part - cut :]

    def columns(row, rows, col, wide):
        return block[:, row : row + rows, col : col + wide].transpose(1, 0, 2).reshape(rows, -1)

    seven = columns(0, 7, 0, part).astype(f32)
    gain_first, shift_first, bias_q, bias_v, bias_o, gain_second, shift_second = seven
    router = columns(0, EXPERTS, 128, part).T
    new_down_b = columns(4, new_count, 128, part)[:, None, :]
    old_down_b = columns(6, new_count, 128, part)[:, None, :]
    new_up_b = columns(0, new_count, 256, new_up_bias.shape[1])[:, None, :]
    old_up_b = columns(2, new_count, 256, new_up_bias.shape[1])[:, None, :]

    flat = tokens.reshape(length, width).astype(f32)
    cot = cotangent.reshape(length, width)
    segments = segment_ids.reshape(length)
    route_flat = routes.reshape(length, -1)
    member = jnp.any(
        route_flat[:, :, None] == jnp.arange(EXPERTS, dtype=jnp.int32)[None, None, :], axis=1
    )
    member_int = member.astype(jnp.int32)
    running = jnp.cumsum(member_int, axis=0)
    position = jnp.where(member, running - 1, -1)
    pos_row = position.T[:, None, :]
    pos_col = position.T[:, :, None]

    unit_one, scale_one = normalize(flat)
    normed = (unit_one * gain_first + shift_first).astype(bf16)
    query = (dot(normed, full_query) + bias_q).astype(bf16)
    keys = dot(normed, full_key).astype(bf16)
    values = (dot(normed, full_value) + bias_v).astype(bf16)
    mixed, probs = attn_forward(query, keys, values, segments[:, None], segments[None, :])
    resid = flat + dot(mixed, full_out) + bias_o
    unit_two, scale_two = normalize(resid)
    normed_two = (unit_two * gain_second + shift_second).astype(bf16)
    logits = dot(normed_two, router)
    trained = (jnp.arange(EXPERTS) >= FROZEN).astype(f32)
    keep = 1.0 - replay.reshape(length, 1).astype(f32) * trained

    def gate_map(values_in):
        gate = jax.nn.softmax(values_in, axis=-1)
        picked = jnp.where(member, gate, 0.0)
        return picked / jnp.sum(picked, axis=-1, keepdims=True) * keep

    share, gate_back = jax.vjp(gate_map, logits)
    share_cols = share.T[:, :, None]

    got = experts(
        True,
        normed_two,
        cot,
        share_cols[FROZEN:],
        pos_row[FROZEN:],
        pos_col[FROZEN:],
        *expert_blocks(new_all, 0, new_count, part, chunks),
        new_up_b,
        new_down_b,
    )
    out_new, gx_new, gc_new, grad_up_b, grad_down_b, packed, side = got
    packed, side = by_owner(packed, side, new_count, part, chunks)
    tall = chunks * part
    summed_new = lax.psum_scatter(
        packed.reshape(-1, width), AXES, scatter_dimension=0, tiled=True
    ).astype(f32)
    middle = tall // 2
    steps_a, steps_b = [], []
    side_sums = [
        scatter_sum(side[:, :middle], one_way, steps_a),
        scatter_sum(side[:, middle:], other_way, steps_b),
    ]
    side_sum = jnp.concatenate(side_sums, axis=0).astype(f32)
    sum_up = jnp.stack([summed_new[:tall], summed_new[2 * tall :]])
    sum_up = sum_up.reshape(new_count, chunks, part, width).transpose(0, 2, 1, 3)
    sum_up = sum_up.reshape(new_count, part, hidden)
    sum_down = jnp.stack([summed_new[tall : 2 * tall], side_sum])

    def frozen(expert, blocks, behind=()):
        here = slice(expert, expert + 1)
        return experts(
            False,
            normed_two,
            cot,
            share_cols[here],
            pos_row[here],
            pos_col[here],
            *blocks,
            old_up_b[here],
            old_down_b[here],
            behind=behind,
        )

    out_first, gx_first, gc_first = frozen(0, expert_blocks(new_all, new_count, 1, part, chunks))
    out_second, gx_second, gc_second = frozen(
        1, expert_blocks(old_all, 0, 1, part, chunks), (steps_a[0], steps_b[0])
    )
    out_old = out_first + out_second
    gx_old = gx_first + gx_second
    gc_old = jnp.concatenate([gc_first, gc_second], axis=0)
    result = (resid + out_new + out_old).astype(bf16)
    grad_share = jnp.concatenate([gc_old, gc_new], axis=0)[:, :, 0].T
    grad_logits = gate_back(grad_share)[0]
    grad_router = lax.dot_general(
        normed_two.astype(f32),
        grad_logits,
        (((0,), (0,)), ((), ())),
        precision=lax.Precision.HIGHEST,
        preferred_element_type=f32,
    )
    grad_two = gx_new + gx_old
    for expert in range(EXPERTS):
        grad_two = grad_two + grad_logits[:, expert : expert + 1] * router[:, expert].astype(f32)
    grad_two = grad_two.astype(bf16).astype(f32)
    grad_gain_two = jnp.sum(grad_two * unit_two, axis=0)
    grad_shift_two = jnp.sum(grad_two, axis=0)
    grad_resid = cot.astype(f32) + normalize_back(unit_two, scale_two, grad_two * gain_second)
    grad_attn = grad_resid.astype(bf16)
    grad_w_out = dot_tn(mixed, grad_attn)
    grad_b_out = jnp.sum(grad_attn.astype(f32), axis=0)
    grad_w_out = grad_w_out.reshape(count, part, width).astype(bf16)
    grad_w_out, grad_attn = lax.optimization_barrier((grad_w_out, grad_attn))
    grad_mixed = dot_nt(grad_attn, full_out).astype(bf16)
    behind = (steps_a[2], steps_b[2])
    grad_q, grad_k, grad_v = attn_backward(query, keys, values, grad_mixed, probs, behind)
    grad_w_query = dot_tn(normed, grad_q)
    grad_w_key = dot_tn(normed, grad_k)
    grad_w_value = dot_tn(normed, grad_v)
    pieces = [
        item.reshape(count, part, width).astype(bf16)
        for item in (grad_w_query, grad_w_key, grad_w_value)
    ]
    last_a = jnp.concatenate([pieces[0], grad_w_out], axis=1)
    last_b = jnp.concatenate(pieces[1:], axis=1)
    last_a, last_b, grad_q, grad_k, grad_v = lax.optimization_barrier(
        (last_a, last_b, grad_q, grad_k, grad_v)
    )
    sum_a = scatter_sum(last_a, one_way).astype(f32)
    grad_b_query = jnp.sum(grad_q.astype(f32), axis=0)
    grad_b_value = jnp.sum(grad_v.astype(f32), axis=0)
    grad_one = dot_nt(grad_q, full_query) + dot_nt(grad_k, full_key) + dot_nt(grad_v, full_value)
    grad_one = grad_one.astype(bf16).astype(f32)
    grad_gain_one = jnp.sum(grad_one * unit_one, axis=0)
    grad_shift_one = jnp.sum(grad_one, axis=0)
    grad_input = grad_resid + normalize_back(unit_one, scale_one, grad_one * gain_first)

    vectors = [grad_gain_one, grad_shift_one, grad_b_query, grad_b_value, grad_b_out]
    vectors += [grad_gain_two, grad_shift_two, grad_router]
    rows = [item.reshape(count, -1) for item in vectors]
    for item in (grad_up_b, grad_down_b):
        rows.append(item.reshape(new_count, count, -1).transpose(1, 0, 2).reshape(count, -1))
    lengths = [item.shape[1] for item in rows]
    row = jnp.concatenate(rows, axis=1).astype(bf16)
    row = jnp.pad(row, ((0, 0), (0, 8 * width - row.shape[1]))).reshape(count, 8, width)
    sum_b = scatter_sum(jnp.concatenate([last_b, row], axis=1), other_way).astype(f32)
    sums = [sum_a[:part], sum_b[:part], sum_b[part : 2 * part], sum_a[part:]]
    tail = sum_b[2 * part]
    found = []
    at = 0
    for size in lengths:
        found.append(tail[at : at + size])
        at += size
    return (
        result.reshape(seqs_here, length, width),
        grad_input.astype(bf16).reshape(seqs_here, length, width),
        found[0],
        found[1],
        sums[0],
        found[2],
        sums[1],
        sums[2],
        found[3],
        sums[3],
        found[4],
        found[5],
        found[6],
        found[7].reshape(part, EXPERTS),
        sum_up,
        found[8].reshape(new_count, -1),
        sum_down,
        found[9].reshape(new_count, -1),
    )


def solution(mesh):
    axes = AXES
    rows3 = P(axes, None, None)
    rows2 = P(axes, None)
    rows1 = P(axes)
    mid3 = P(None, axes, None)
    mid2 = P(None, axes)
    placed = (rows3, rows3, rows2, rows3, rows2)
    placed += (rows1, rows1, rows2, rows1, rows2, rows2, rows1, rows2, rows1, rows1, rows1, rows2)
    placed += (mid3, mid2) * 4
    outs = (rows3, rows3, rows1, rows1, rows2, rows1, rows2, rows2, rows1, rows2, rows1)
    outs += (rows1, rows1, rows2, mid3, mid2, mid3, mid2)
    return jax.shard_map(local, mesh=mesh, in_specs=placed, out_specs=outs, check_vma=False)
```
